512 devices in a mesh: tm: 32 (over y, z_lo), space: 16 (over x, z_hi, core).
Axes of the slice: x: 4, y: 8, z: 8 (z_hi: 2, z_lo: 4; z = z_hi * 4 + z_lo), core: 2. Of those that a mesh axis runs over, the one named last changes fastest.
Arguments:
- c_points: float32 [32, 256, 32, 128], P('tm', 'space'), may hold values from -15 to 15
- corrections: float32 [32, 256, 32, 128], P('tm', 'space'), may hold values from -3 to 3
- conductivity: float32 [256, 32, 128], P('space'), may hold values from 0.2 to 5
- forcing: float32 [256, 32, 128], P('space'), may hold values from -6 to 6
Outputs:
- f_states: float32 [32, 2, 256, 32, 128], P('tm', None, 'space')
The draws below stay inside these ranges and needn't reach their ends.
All inputs are finite; a program needn't handle non-finite values.
Results may differ from the reference program's by a relative error of at most 0.0002.
Values sent between devices are 32-bit elements; how exact they have to be, the bound alone decides.
No kernel may reach another device: no remote copies, remote signals or barrier semaphores. Data moves between devices by JAX's collectives and lax.ppermute only.
A program may use at most 64 MiB of HBM per device.

```python
import math
import jax
import jax.numpy as jnp
from jax import lax

NY = 32
NX = 128
ITERS = 6
STEPS = 2
GROUPS = 32
NZ = 256


def draw_c_points(key, part):
    depth_frac = jnp.arange(NZ, dtype=jnp.float32) / max(NZ - 1, 1)
    depth_scale = (1.0 + 2.0 * depth_frac)[None, :, None, None]
    random_part = jax.random.normal(key, (GROUPS, NZ, NY, NX), jnp.float32)
    values = depth_scale * random_part
    return jnp.clip(values, -15.0, 15.0)


def block_levels(key, shape, cuts, smallest, largest):
    factor_of = 1.0
    for dim, parts in cuts:
        heights = jax.random.uniform(jax.random.fold_in(jax.random.fold_in(key, 6), dim), (parts,), jnp.float32, smallest / len(cuts), largest / len(cuts))
        factor_of = factor_of * jnp.repeat(jnp.exp(heights), shape[dim] // parts).reshape((-1,) + (1,) * (len(shape) - 1 - dim))
    return factor_of


def gaussian(key, extent, spread, most, shards=(), kind=jnp.bfloat16):
    factor_of = block_levels(key, extent, shards, -0.22, 0.18) if shards else 1.0
    entries = jax.random.normal(key, extent, jnp.float32) * spread * factor_of
    return jnp.minimum(jnp.maximum(entries, -most), most).astype(kind)


def setup_inputs(seed: int = 0) -> dict:
    keys = jax.random.split(jax.random.key(seed), 5)
    return {
        "c_points": draw_c_points(jax.random.fold_in(keys[4], 71), 0),
        "corrections": gaussian(keys[1], (GROUPS, NZ, NY, NX), 0.5, 3.0, ((0, 32), (1, 16)), jnp.float32),
        "conductivity": jnp.clip(jnp.exp(math.log(5.0) - 3.218876 * jax.random.uniform(keys[2], (NZ, NY, NX), jnp.float32) ** block_levels(keys[2], (NZ, NY, NX), ((0, 16),), -0.2, 0.2)), 0.2, 5.0),
        "forcing": gaussian(keys[3], (NZ, NY, NX), 1.0, 6.0, ((0, 16),), jnp.float32),
    }


step_rate = 4.0
source_weight = 0.25


def neighbours(padded):
    return (padded[2:, 1:-1, 1:-1], padded[:-2, 1:-1, 1:-1],
            padded[1:-1, 2:, 1:-1], padded[1:-1, :-2, 1:-1],
            padded[1:-1, 1:-1, 2:], padded[1:-1, 1:-1, :-2])


def faces_of(padded_conductivity):
    centre = padded_conductivity[1:-1, 1:-1, 1:-1]
    return tuple(0.5 * (centre + beside) for beside in neighbours(padded_conductivity))


def apply_operator(grid_field, padded, face_weights):
    flux_sum = jnp.zeros_like(grid_field)
    for face_weight, beside in zip(face_weights, neighbours(padded)):
        flux_sum = flux_sum + face_weight * (grid_field - beside)
    return grid_field + step_rate * flux_sum


def reference(c_points, corrections, conductivity, forcing):
    face_weights = faces_of(jnp.pad(conductivity, 1))

    def operate(grid_field):
        return apply_operator(grid_field, jnp.pad(grid_field, 1), face_weights)

    def advance(start_value):
        current = start_value
        sections = []
        for section in range(STEPS):
            right_side = current + source_weight * forcing
            solution = current
            residual = right_side - operate(current)
            direction = residual
            norm_now = jnp.sum(residual * residual)
            for sweep in range(ITERS):
                applied = operate(direction)
                step_length = norm_now / jnp.sum(direction * applied)
                solution = solution + step_length * direction
                if sweep + 1 < ITERS:
                    residual = residual - step_length * applied
                    norm_next = jnp.sum(residual * residual)
                    direction = residual + (norm_next / norm_now) * direction
                    norm_now = norm_next
            sections.append(solution)
            current = solution
        return jnp.stack(sections)

    prior_fix = jnp.concatenate([jnp.zeros_like(corrections[:1]), corrections[:-1]], axis=0)
    start_values = c_points + prior_fix
    return lax.map(advance, start_values)
```

```python
import jax
import jax.numpy as jnp
from jax import lax
from jax.experimental import pallas as pl
from jax.experimental.pallas import tpu as pltpu
from jax.sharding import PartitionSpec as P

ITERS = 6
STEPS = 2
STEP_RATE = 4.0
SOURCE_WEIGHT = 0.25


LOW, HIGH = 1.0, 160.0
MID = 0.5 * (LOW + HIGH)
HALF = 0.5 * (HIGH - LOW)
SIGMA = 2.0 / HALF
KAPPA = SIGMA * (1.0 - MID)
FACE = 0.5 * STEP_RATE * SIGMA

RIM = ITERS
SUB = 8
LANES = 128
PAIRS = [(i, j) for j in range(ITERS) for i in range(j + 1)]
TOTALS = len(PAIRS) + 1
GROUPS_OF_8 = (TOTALS + 7) // 8
TINY_PIVOT = 1e-9


def two_sum(a, b):
    s = a + b
    t = s - a
    return s, (a - (s - t)) + (b - t)


def quick_two_sum(a, b):
    s = a + b
    return s, b - (s - a)


def add2(a, b):
    s, e = two_sum(a[0], b[0])
    return quick_two_sum(s, e + (a[1] + b[1]))


def neg2(a):
    return -a[0], -a[1]


def split(a):
    t = 4097.0 * a
    hi = t - (t - a)
    return hi, a - hi


def two_prod(a, b):
    p = a * b
    ah, al = split(a)
    bh, bl = split(b)
    return p, ((ah * bh - p) + ah * bl + al * bh) + al * bl


def mul2(a, b):
    p, e = two_prod(a[0], b[0])
    return quick_two_sum(p, e + (a[0] * b[1] + a[1] * b[0]))


def scale2(a, c):
    hi = jnp.full_like(a[0], c[0])
    lo = jnp.full_like(a[0], c[1])
    return mul2(a, (hi, lo))


def const2(c):
    import numpy as np

    hi = float(np.float32(c))
    return hi, float(np.float32(c - hi))


def recip2(a):
    q = 1.0 / a[0]
    p, e = two_prod(q, a[0])
    r = (1.0 - p) - (e + q * a[1])
    return quick_two_sum(q, q * r)


def roll(v, shift, axis):
    return pltpu.roll(v, shift % v.shape[axis], axis)


def load_rows(ref, z, k):
    return ref[z, pl.ds(k, SUB, stride=4), :]


def divergence(load, weights, first, last, emit):
    wz, wy, wx = weights
    below = load(first - 1)
    here = load(first)
    flux_below = [wz[first - 1, k] * (here[k] - below[k]) for k in range(4)]
    for e in range(first, last + 1):
        above = load(e + 1)
        flux_above = [wz[e, k] * (above[k] - here[k]) for k in range(4)]
        fx = [wx[e, k] * (roll(here[k], -1, 1) - here[k]) for k in range(4)]
        nxt = [here[1], here[2], here[3], roll(here[0], -1, 0)]
        fy = [wy[e, k] * (nxt[k] - here[k]) for k in range(4)]
        prv = [roll(fy[3], 1, 0), fy[0], fy[1], fy[2]]
        div = [
            (flux_above[k] - flux_below[k]) + (fy[k] - prv[k]) + (fx[k] - roll(fx[k], 1, 1)) for k in range(4)
        ]
        emit(e, here, div)
        here, flux_below = above, flux_above


def planes(ref, *lead):
    return lambda e: [ref[(*lead, e, k)] for k in range(4)]


def krylov(basis, weights, diag, span, inside):
    own_first, own_last = RIM + 1, span - RIM - 2

    def mask(k):
        for e, m in ((own_first - 1, inside[0]), (own_last + 1, inside[1])):
            for q in range(4):
                basis[k, e, q] = basis[k, e, q] * m

    mask(0)
    for k in range(1, ITERS):

        def emit(e, v, div, k=k):
            for q in range(4):
                image = diag[e, q] * v[q] - div[q]
                basis[k, e, q] = 0.5 * image if k == 1 else image - basis[k - 2, e, q]

        divergence(planes(basis, k - 1), weights, 1 + k, span - 2 - k, emit)
        mask(k)
    sums = {}

    def take(key, terms):
        s = (terms[0] + terms[1]) + (terms[2] + terms[3])
        if key in sums:
            hi, e = two_sum(sums[key][0], s)
            sums[key] = (hi, sums[key][1] + e)
        else:
            sums[key] = (s, jnp.zeros_like(s))

    def last(e, v, div):
        take("q", [v[q] * (diag[e, q] * v[q] - div[q]) for q in range(4)])

    divergence(planes(basis, ITERS - 1), weights, own_first, own_last, last)
    for chunk in ([(i, 5) for i in range(6)], [(i, j) for i, j in PAIRS if 3 <= j <= 4], [(i, j) for i, j in PAIRS if j < 3]):
        for e in range(own_first, own_last + 1):
            used = sorted({i for pair in chunk for i in pair})
            v = {i: [basis[i, e, q] for q in range(4)] for i in used}
            for i, j in chunk:
                take((i, j), [v[i][q] * v[j][q] for q in range(4)])
    return [sums[p] for p in PAIRS] + [sums["q"]]


def pack(totals, out):
    for shift in (4, 2, 1):
        totals = [add2(t, (roll(t[0], shift, 0), roll(t[1], shift, 0))) for t in totals]
    row = lax.broadcasted_iota(jnp.int32, (SUB, LANES), 0)
    lane = lax.broadcasted_iota(jnp.int32, (SUB, LANES), 1)
    result = jnp.zeros((SUB, LANES), jnp.float32)
    for g in range(GROUPS_OF_8):
        part = totals[8 * g : 8 * g + 8]
        hi = lo = jnp.zeros((SUB, LANES), jnp.float32)
        for i, t in enumerate(part):
            hi = jnp.where(row == i, t[0], hi)
            lo = jnp.where(row == i, t[1], lo)
        both = (hi, lo)
        for shift in (64, 32, 16, 8, 4, 2, 1):
            both = add2(both, (roll(both[0], shift, 1), roll(both[1], shift, 1)))
        result = jnp.where(lane == g, both[0], result)
        result = jnp.where(lane == GROUPS_OF_8 + g, both[1], result)
    for p in range(out.shape[0]):
        out[p] = result


def unpack(gathered):
    hi = gathered[0]
    lo = jnp.zeros_like(hi)
    for p in range(1, gathered.shape[0]):
        hi, e = two_sum(hi, gathered[p])
        lo = lo + e
    lo = lo + roll(hi, -GROUPS_OF_8, 1)
    hi, lo = quick_two_sum(hi, lo)
    totals = []
    for i in range(TOTALS):
        s, g = i % 8, i // 8
        totals.append(
            (
                jnp.broadcast_to(hi[s : s + 1, g : g + 1], (SUB, LANES)),
                jnp.broadcast_to(lo[s : s + 1, g : g + 1], (SUB, LANES)),
            )
        )
    return totals


def galerkin(totals):
    b = {}
    for p, t in zip(PAIRS, totals):
        b[p] = t
        b[p[::-1]] = t
    mid, half2 = const2(MID), const2(0.5 * HALF)
    m = {}
    for j in range(ITERS):
        for i in range(j + 1):
            if i == ITERS - 1:
                q = totals[-1]
            elif i == 0:
                q = (2.0 * b[1, j][0], 2.0 * b[1, j][1])
            else:
                q = add2(b[i + 1, j], b[i - 1, j])
            m[j, i] = add2(scale2(q, half2), scale2(b[i, j], mid))
    y = [b[0, i] for i in range(ITERS)]
    inverse = []
    unit = {}
    least = None
    diagonal = [m[i, i][0] for i in range(ITERS)]
    for j in range(ITERS):
        whole = diagonal[j]
        good = m[j, j][0] > TINY_PIVOT * whole
        ratio = m[j, j][0] / whole
        least = ratio if least is None else jnp.minimum(least, ratio)
        inv = recip2((jnp.where(good, m[j, j][0], 1.0), jnp.where(good, m[j, j][1], 0.0)))
        inv = (jnp.where(good, inv[0], 0.0), jnp.where(good, inv[1], 0.0))
        inverse.append(inv)
        for i in range(j + 1, ITERS):
            unit[i, j] = mul2(m[i, j], inv)
        for i in range(j + 1, ITERS):
            minus = neg2(unit[i, j])
            for k in range(j + 1, i + 1):
                m[i, k] = add2(m[i, k], mul2(minus, m[k, j]))
            y[i] = add2(y[i], mul2(minus, y[j]))
    c = [mul2(y[j], inverse[j])[0] for j in range(ITERS)]
    for j in reversed(range(ITERS)):
        for i in range(j + 1, ITERS):
            c[j] = c[j] - unit[i, j][0] * c[i]
    return c, least


def start_kernel(c, k, f, a, lo, hi, klo, khi, basis, x, wz, wy, wx, bd, sums, cond, diag):
    depth = c.shape[0]
    rim = RIM + 1
    span = depth + 2 * rim
    forcing = {}

    def put(e, z, point, fix, source, conduct):
        for q in range(4):
            x[e, q] = load_rows(*point, q) + load_rows(*fix, q)
            cond[e, q] = load_rows(*conduct, q)

    for z in range(rim):
        put(z, z, (lo, z), (klo, z), None, (lo, rim + RIM + z))
        put(rim + depth + z, z, (hi, z), (khi, z), None, (hi, rim + RIM + z))
    for z in range(depth):
        put(rim + z, z, (c, z), (k, z), None, (a, z))

    def source(e, q):
        if e < rim:
            return load_rows(lo, rim + e - 1, q)
        if e < rim + depth:
            return load_rows(f, e - rim, q)
        return load_rows(hi, rim + e - rim - depth, q)

    row = lax.broadcasted_iota(jnp.int32, (SUB, LANES), 0)
    lane = lax.broadcasted_iota(jnp.int32, (SUB, LANES), 1)
    not_last_lane = jnp.where(lane < LANES - 1, FACE, 0.0)
    not_last_row = jnp.where(row < SUB - 1, FACE, 0.0)
    side = jnp.where((lane == 0) | (lane == LANES - 1), FACE, 0.0)
    edge = [side + jnp.where(row == 0, FACE, 0.0), side, side, side + jnp.where(row == SUB - 1, FACE, 0.0)]
    here = [cond[0, q] for q in range(4)]
    for e in range(span - 1):
        above = [cond[e + 1, q] for q in range(4)]
        for q in range(4):
            wz[e, q] = FACE * (here[q] + above[q])
        if e > 0:
            nxt = [here[1], here[2], here[3], roll(here[0], -1, 0)]
            for q in range(4):
                wx[e, q] = not_last_lane * (here[q] + roll(here[q], -1, 1))
                wy[e, q] = (FACE if q < 3 else not_last_row) * (here[q] + nxt[q])
                bound = edge[q] * here[q]
                bd[e, q] = bound
                diag[e, q] = KAPPA + bound
        here = above

    def emit(e, v, div):
        for q in range(4):
            basis[0, e, q] = SOURCE_WEIGHT * source(e, q) - (1.0 / SIGMA) * (bd[e, q] * v[q] - div[q])

    divergence(planes(x), (wz, wy, wx), 1, span - 2, emit)
    inside = (
        jnp.where(cond[rim - 1, 0] > 0, 1.0, 0.0),
        jnp.where(cond[rim + depth, 0] > 0, 1.0, 0.0),
    )
    pack(krylov(basis, (wz, wy, wx), diag, span, inside), sums)


def middle_kernel(gathered, basis, x, f, wz, wy, wx, bd, state, res, head, tail, flag, wide):
    depth = f.shape[0]
    rim = RIM + 1
    c, least = galerkin(unpack(gathered))
    flag[...] = least
    for e in range(rim - 1, rim + depth + 1):
        for q in range(4):
            s = x[e, q]
            for i in range(ITERS):
                s = s + c[i] * basis[i, e, q]
            wide[e, q] = s
            if rim <= e < rim + depth:
                state[e - rim, q] = s

    def emit(e, v, div):
        z = e - rim
        for q in range(4):
            r = SOURCE_WEIGHT * load_rows(f, z, q) - (1.0 / SIGMA) * (bd[e, q] * v[q] - div[q])
            res[z, q] = r
            if z < RIM:
                head[z, q] = r
            if z >= depth - RIM:
                tail[z - depth + RIM, q] = r

    divergence(planes(wide), (wz, wy, wx), rim, rim + depth - 1, emit)


def again_kernel(res, lo, hi, wz, wy, wx, bd, basis, sums, diag):
    depth = res.shape[0]
    rim = RIM + 1
    span = depth + 2 * rim
    for e in range(1, span - 1):
        for q in range(4):
            diag[e, q] = KAPPA + bd[e, q]
            if e < rim:
                v = lo[e - 1, q]
            elif e < rim + depth:
                v = res[e - rim, q]
            else:
                v = hi[e - rim - depth, q]
            basis[0, e, q] = v
    one = jnp.ones((SUB, LANES), jnp.float32)
    inside = (
        jnp.where(wz[rim - 2, 0] > 0, one, 0.0),
        jnp.where(wz[rim + depth, 0] > 0, one, 0.0),
    )
    pack(krylov(basis, (wz, wy, wx), diag, span, inside), sums)


def end_kernel(gathered, basis, state, flag_in, out, flag):
    depth = state.shape[0]
    rim = RIM + 1
    c, least = galerkin(unpack(gathered))
    flag[...] = jnp.minimum(least, flag_in[...])
    for z in range(depth):
        for q in range(4):
            s = state[z, q]
            out[0, 0, z, pl.ds(q, SUB, stride=4), :] = s
            for i in range(ITERS):
                s = s + c[i] * basis[i, z + rim, q]
            out[0, 1, z, pl.ds(q, SUB, stride=4), :] = s


def call(kernel, outs, scratch=()):
    shapes = [jax.ShapeDtypeStruct(s, jnp.float32) for s in outs]
    return pl.pallas_call(
        kernel,
        out_shape=shapes,
        scratch_shapes=[pltpu.VMEM(s, jnp.float32) for s in scratch],
        compiler_params=pltpu.CompilerParams(vmem_limit_bytes=48 * 2**20),
    )


def exchange(sums):
    return lax.all_to_all(sums, "space", 0, 0, tiled=True)


def body(c_points, corrections, conductivity, forcing):
    times, slabs = lax.axis_size("tm"), lax.axis_size("space")
    own_point, own_fix = c_points[0], corrections[0]
    depth = own_point.shape[0]
    rim = RIM + 1
    span = depth + 2 * rim
    tile = (4, SUB, LANES)
    up = [(i, i + 1) for i in range(slabs - 1)]
    down = [(i + 1, i) for i in range(slabs - 1)]
    later = [(i, i + 1) for i in range(times - 1)]
    both = ("tm", "space")

    def across(moves):
        return [(t * slabs + s, (t + 1) * slabs + d) for t in range(times - 1) for s, d in moves]

    fix = lax.ppermute(own_fix, "tm", later)
    tail = jnp.concatenate([own_point[-rim:], forcing[-RIM:], conductivity[-rim:]])
    head = jnp.concatenate([own_point[:rim], forcing[:RIM], conductivity[:rim]])
    lo = lax.ppermute(tail, "space", up)
    hi = lax.ppermute(head, "space", down)
    fix_lo = lax.ppermute(own_fix[-rim:], both, across(up))
    fix_hi = lax.ppermute(own_fix[:rim], both, across(down))

    field = (span, *tile)
    basis_shape = (ITERS, *field)
    sums_shape = (slabs, SUB, LANES)
    basis, x, wz, wy, wx, bd, sums = call(
        start_kernel,
        [basis_shape, field, field, field, field, field, sums_shape],
        [field, field],
    )(own_point, fix, forcing, conductivity, lo, hi, fix_lo, fix_hi)
    sums = exchange(sums)
    part = (depth, *tile)
    rim_shape = (RIM, *tile)
    state, res, head, tail, flag = call(
        middle_kernel, [part, part, rim_shape, rim_shape, (SUB, LANES)], [field]
    )(sums, basis, x, forcing, wz, wy, wx, bd)
    lo = lax.ppermute(tail, "space", up)
    hi = lax.ppermute(head, "space", down)
    basis, sums = call(again_kernel, [basis_shape, sums_shape], [field])(res, lo, hi, wz, wy, wx, bd)
    sums = exchange(sums)
    out, flag = call(end_kernel, [(1, STEPS, depth, 32, LANES), (SUB, LANES)])(sums, basis, state, flag)
    return out


def solution(mesh):
    in_specs = (
        P("tm", "space", None, None),
        P("tm", "space", None, None),
        P("space", None, None),
        P("space", None, None),
    )
    out_specs = P("tm", None, "space", None, None)
    return jax.shard_map(body, mesh=mesh, in_specs=in_specs, out_specs=out_specs, check_vma=False)
```

```python
import jax
import jax.numpy as jnp
import numpy as np
from jax import lax
from jax.experimental import pallas as pl
from jax.experimental.pallas import tpu as pltpu
from jax.sharding import PartitionSpec as P

ITERS = 6
STEPS = 2
STEP_RATE = 4.0
SOURCE_WEIGHT = 0.25


LOW, HIGH = 1.0, 141.0
MID = 0.5 * (LOW + HIGH)
HALF = 0.5 * (HIGH - LOW)
SIGMA = 2.0 / HALF
KAPPA = SIGMA * (1.0 - MID)
FACE = 0.5 * STEP_RATE * SIGMA

TERMS = STEPS * ITERS
RIM = TERMS + 1
SUB = 8
LANES = 128
TOTALS = 2 * TERMS + 1 + ITERS
GROUPS_OF_8 = (TOTALS + 7) // 8
NOISE = 1e-8
ALLOWED = 5e-5


def two_sum(a, b):
    s = a + b
    t = s - a
    return s, (a - (s - t)) + (b - t)


def quick_two_sum(a, b):
    s = a + b
    return s, b - (s - a)


def add2(a, b):
    s, e = two_sum(a[0], b[0])
    return quick_two_sum(s, e + (a[1] + b[1]))


def neg2(a):
    return -a[0], -a[1]


def split(a):
    t = 4097.0 * a
    hi = t - (t - a)
    return hi, a - hi


def two_prod(a, b):
    p = a * b
    ah, al = split(a)
    bh, bl = split(b)
    return p, ((ah * bh - p) + ah * bl + al * bh) + al * bl


def mul2(a, b):
    p, e = two_prod(a[0], b[0])
    return quick_two_sum(p, e + (a[0] * b[1] + a[1] * b[0]))


def const2(c):
    hi = float(np.float32(c))
    return hi, float(np.float32(c - hi))


def recip2(a):
    q = 1.0 / a[0]
    p, e = two_prod(q, a[0])
    r = (1.0 - p) - (e + q * a[1])
    return quick_two_sum(q, q * r)


def roll(v, shift, axis):
    return pltpu.roll(v, shift % v.shape[axis], axis)


def load_rows(ref, z, k):
    return ref[z, pl.ds(k, SUB, stride=4), :]


def times2(a, c):
    hi, lo = const2(c)
    return mul2(a, (jnp.full_like(a[0], hi), jnp.full_like(a[0], lo)))


def double2(a):
    return 2.0 * a[0], 2.0 * a[1]


def half2(a):
    return 0.5 * a[0], 0.5 * a[1]


def divergence(load, weights, first, last, emit):
    wz, wy, wx = weights
    below = load(first - 1)
    here = load(first)
    flux_below = [wz[first - 1, k] * (here[k] - below[k]) for k in range(4)]
    for e in range(first, last + 1):
        above = load(e + 1)
        flux_above = [wz[e, k] * (above[k] - here[k]) for k in range(4)]
        fx = [wx[e, k] * (roll(here[k], -1, 1) - here[k]) for k in range(4)]
        nxt = [here[1], here[2], here[3], roll(here[0], -1, 0)]
        fy = [wy[e, k] * (nxt[k] - here[k]) for k in range(4)]
        prv = [roll(fy[3], 1, 0), fy[0], fy[1], fy[2]]
        div = [
            (flux_above[k] - flux_below[k]) + (fy[k] - prv[k]) + (fx[k] - roll(fx[k], 1, 1)) for k in range(4)
        ]
        emit(e, here, div)
        here, flux_below = above, flux_above


def planes(ref, *lead):
    return lambda e: [ref[(*lead, e, k)] for k in range(4)]


def pack(totals, out):
    for shift in (4, 2, 1):
        totals = [add2(t, (roll(t[0], shift, 0), roll(t[1], shift, 0))) for t in totals]
    row = lax.broadcasted_iota(jnp.int32, (SUB, LANES), 0)
    lane = lax.broadcasted_iota(jnp.int32, (SUB, LANES), 1)
    result = jnp.zeros((SUB, LANES), jnp.float32)
    for g in range(GROUPS_OF_8):
        part = totals[8 * g : 8 * g + 8]
        hi = lo = jnp.zeros((SUB, LANES), jnp.float32)
        for i, t in enumerate(part):
            hi = jnp.where(row == i, t[0], hi)
            lo = jnp.where(row == i, t[1], lo)
        both = (hi, lo)
        for shift in (64, 32, 16, 8, 4, 2, 1):
            both = add2(both, (roll(both[0], shift, 1), roll(both[1], shift, 1)))
        result = jnp.where(lane == g, both[0], result)
        result = jnp.where(lane == GROUPS_OF_8 + g, both[1], result)
    for p in range(out.shape[0]):
        out[p] = result


def unpack(gathered):
    hi = gathered[0]
    lo = jnp.zeros_like(hi)
    for p in range(1, gathered.shape[0]):
        hi, e = two_sum(hi, gathered[p])
        lo = lo + e
    lo = lo + roll(hi, -GROUPS_OF_8, 1)
    hi, lo = quick_two_sum(hi, lo)
    whole = (SUB, LANES)
    spot = lambda v, i: jnp.broadcast_to(v[i % 8 : i % 8 + 1, i // 8 : i // 8 + 1], whole)
    return [(spot(hi, i), spot(lo, i)) for i in range(TOTALS)]


def galerkin(nu):
    image = []
    for k in range(2 * ITERS - 1):
        image.append(add2(times2(nu[k], MID), times2(add2(nu[k + 1], nu[abs(k - 1)]), 0.5 * HALF)))
    m = {(i, j): half2(add2(image[i + j], image[i - j])) for i in range(ITERS) for j in range(i + 1)}
    y = [nu[i] for i in range(ITERS)]
    inverse, unit = [], {}
    for j in range(ITERS):
        inverse.append(recip2(m[j, j]))
        for i in range(j + 1, ITERS):
            unit[i, j] = mul2(m[i, j], inverse[j])
        for i in range(j + 1, ITERS):
            minus = neg2(unit[i, j])
            for k in range(j + 1, i + 1):
                m[i, k] = add2(m[i, k], mul2(minus, m[k, j]))
            y[i] = add2(y[i], mul2(minus, y[j]))
    c = [mul2(y[j], inverse[j])[0] for j in range(ITERS)]
    for j in reversed(range(ITERS)):
        for i in range(j + 1, ITERS):
            c[j] = c[j] - unit[i, j][0] * c[i]
    return c


def next_moments(nu, c):
    zero = jnp.zeros_like(c[0])
    shifted = [(zero, zero)] * (ITERS + 2)

    def put(k, v):
        shifted[k] = add2(shifted[k], v)

    for k, v in enumerate(c):
        put(k + 1, (v if k == 0 else 0.5 * v, zero))
        if k > 0:
            put(k - 1, (0.5 * v, zero))
    q = []
    for k in range(ITERS + 1):
        u = times2(shifted[k], -HALF)
        if k < ITERS:
            u = add2(u, times2((c[k], zero), 1.0 - MID))
        q.append(add2((jnp.ones_like(zero), zero), u) if k == 0 else u)
    square = [(zero, zero)] * (2 * ITERS + 1)

    def gather(k, v):
        square[k] = v if square[k][0] is zero else add2(square[k], v)

    for i in range(ITERS + 1):
        for j in range(i + 1):
            v = mul2(q[i], q[j])
            if i == j:
                v = half2(v)
            gather(i + j, v)
            gather(i - j, v)
    result = []
    for k in range(2 * ITERS):
        total = None
        for i in range(2 * ITERS + 1):
            v = mul2(square[i], half2(add2(nu[i + k], nu[abs(i - k)])))
            total = v if total is None else add2(total, v)
        result.append(total)
    return result


def solve(totals):
    row = lax.broadcasted_iota(jnp.int32, (SUB, LANES), 0)
    shaken = []
    for i in range(2 * TERMS):
        sign = jnp.where((row * (2 * i + 3) * 5 + i * 3 + row * row * (i + 1)) % 7 < 3, NOISE, -NOISE)
        sign = jnp.where(row == 0, 0.0, sign)
        scale = totals[i - i % 2][0]
        shaken.append(quick_two_sum(totals[i][0], totals[i][1] + sign * scale))
    nu = []
    for i in range(2 * TERMS):
        nu.append(shaken[i] if i < 2 else add2(double2(shaken[i]), neg2(nu[i % 2])))
    c1 = galerkin(nu)
    nu2 = next_moments(nu, c1)
    c2 = galerkin(nu2)

    def proper(v):
        return jnp.broadcast_to(v[0:1], v.shape)

    def energy(d, m):
        total = None
        for i in range(ITERS):
            for j in range(i + 1):
                v = d[i] * d[j] * (m[i + j][0] + m[i - j][0])
                v = 0.5 * v if i == j else v
                total = v if total is None else total + v
        return total

    best1, best2 = [proper(v) for v in c1], [proper(v) for v in c2]
    moved = energy([a - b for a, b in zip(c1, best1)], nu) + energy([a - b for a, b in zip(c2, best2)], nu2)
    size = totals[2 * TERMS][0] + energy(best1, nu)
    for i in range(ITERS):
        size = size + 2.0 * best1[i] * totals[2 * TERMS + 1 + i][0]
    good = jnp.where(moved <= ALLOWED**2 * size, 1.0, 0.0)
    for shift in (4, 2, 1):
        good = jnp.minimum(good, roll(good, shift, 0))
    return best1, best2, good


def states_kernel(gathered, basis, x0, xlo, xhi, f, flo, fhi, wz, wy, wx, bd, out, flag, wide, ring, final):
    depth = x0.shape[0]
    span = depth + 2 * RIM
    keep = RIM - ITERS
    weights = (wz, wy, wx)
    mask = inside(wz, depth)
    c1, c2, good = solve(unpack(gathered))
    flag[...] = good
    for e in range(keep, span - keep):
        ref, z = at(e, xlo, x0, xhi, depth, RIM)
        for q in range(4):
            s = load_rows(ref, z, q)
            for i in range(ITERS):
                s = s + c1[i] * basis[i, e - keep, q]
            wide[e, q] = s
            if RIM <= e < RIM + depth:
                out[0, 0, e - RIM, pl.ds(q, SUB, stride=4), :] = s

    def store(k, e, new):
        if e in mask:
            new = [n * mask[e] for n in new]
        for q in range(4):
            if k < ITERS - 1:
                ring[k % 3, e, q] = new[q]
            if RIM <= e < RIM + depth:
                before = wide[e, q] if k == 0 else final[e - RIM, q]
                s = before + c2[k] * new[q]
                if k < ITERS - 1:
                    final[e - RIM, q] = s
                else:
                    out[0, 1, e - RIM, pl.ds(q, SUB, stride=4), :] = s

    def first(e, v, div):
        ref, z = at(e - 1, flo, f, fhi, depth, TERMS)
        store(
            0,
            e,
            [SOURCE_WEIGHT * load_rows(ref, z, q) - (1.0 / SIGMA) * (bd[e, q] * v[q] - div[q]) for q in range(4)],
        )

    divergence(planes(wide), weights, keep + 1, span - keep - 2, first)
    for k in range(1, ITERS):

        def emit(e, v, div, k=k):
            image = [(KAPPA + bd[e, q]) * v[q] - div[q] for q in range(4)]
            if k == 1:
                new = [0.5 * i for i in image]
            else:
                new = [i - ring[(k - 2) % 3, e, q] for q, i in enumerate(image)]
            store(k, e, new)

        divergence(planes(ring, (k - 1) % 3), weights, keep + 1 + k, span - keep - 2 - k, emit)


def call(kernel, outs, scratch=()):
    shapes = [jax.ShapeDtypeStruct(s, jnp.float32) for s in outs]
    return pl.pallas_call(
        kernel,
        out_shape=shapes,
        scratch_shapes=[pltpu.VMEM(s, jnp.float32) for s in scratch],
        compiler_params=pltpu.CompilerParams(vmem_limit_bytes=48 * 2**20),
    )


def fast(c_points, corrections, conductivity, forcing):
    times, slabs = lax.axis_size("tm"), lax.axis_size("space")
    own_point, own_fix = c_points[0], corrections[0]
    depth = own_point.shape[0]
    span = depth + 2 * RIM
    tile = (4, SUB, LANES)
    up = [(i, i + 1) for i in range(slabs - 1)]
    down = [(i + 1, i) for i in range(slabs - 1)]
    later = [(i, i + 1) for i in range(times - 1)]

    def short(moves):
        pairs = []
        for t in range(times):
            for s, d in moves:
                u = t if (s // 2) % 2 == (d // 2) % 2 else t // 4 * 4 + 3 - t % 4
                pairs.append((t * slabs + s, u * slabs + d))
        return pairs

    fix = lax.ppermute(own_fix, "tm", later)
    flo = lax.ppermute(jnp.concatenate([forcing[-TERMS:], conductivity[-RIM:]]), ("tm", "space"), short(up))
    fhi = lax.ppermute(jnp.concatenate([forcing[:TERMS], conductivity[:RIM]]), ("tm", "space"), short(down))
    x0 = own_point + fix
    xlo = lax.ppermute(x0[-RIM:], "space", up)
    xhi = lax.ppermute(x0[:RIM], "space", down)
    field = (span, *tile)
    wz, wy, wx, bd = call(weights_kernel, [field] * 4)(conductivity, flo, fhi)
    inputs = (x0, xlo, xhi, forcing, flo, fhi, wz, wy, wx, bd)
    kept = depth + 2 * ITERS
    basis, sums = call(basis_kernel, [(ITERS, kept, *tile), (slabs, SUB, LANES)], [(3, *field)])(*inputs)
    sums = lax.all_to_all(sums, "space", 0, 0, tiled=True)
    return call(
        states_kernel,
        [(1, STEPS, depth, 4 * SUB, LANES), (SUB, LANES)],
        [field, (3, *field), (depth, *tile)],
    )(sums, basis, *inputs)


def at(e, low, own, high, depth, rim):
    if e < rim:
        return low, e
    if e < rim + depth:
        return own, e - rim
    return high, e - rim - depth


def weights_kernel(a, lo, hi, wz, wy, wx, bd):
    depth = a.shape[0]
    span = depth + 2 * RIM
    row = lax.broadcasted_iota(jnp.int32, (SUB, LANES), 0)
    lane = lax.broadcasted_iota(jnp.int32, (SUB, LANES), 1)
    not_last_lane = jnp.where(lane < LANES - 1, FACE, 0.0)
    not_last_row = jnp.where(row < SUB - 1, FACE, 0.0)
    side = jnp.where((lane == 0) | (lane == LANES - 1), FACE, 0.0)
    edge = [side + jnp.where(row == 0, FACE, 0.0), side, side, side + jnp.where(row == SUB - 1, FACE, 0.0)]

    def conduct(e):
        ref, z = at(e, lo, a, hi, depth, RIM)
        return [load_rows(ref, z if ref is a else z + TERMS, q) for q in range(4)]

    here = conduct(0)
    for e in range(span):
        if e + 1 < span:
            above = conduct(e + 1)
            for q in range(4):
                wz[e, q] = FACE * (here[q] + above[q])
        nxt = [here[1], here[2], here[3], roll(here[0], -1, 0)]
        for q in range(4):
            wx[e, q] = not_last_lane * (here[q] + roll(here[q], -1, 1))
            wy[e, q] = (FACE if q < 3 else not_last_row) * (here[q] + nxt[q])
            bd[e, q] = edge[q] * here[q]
        here = above


def inside(wz, depth):
    one = jnp.ones((SUB, LANES), jnp.float32)
    return {
        RIM - 1: jnp.where(wz[RIM - 2, 0] > 0, one, 0.0),
        RIM + depth: jnp.where(wz[RIM + depth, 0] > 0, one, 0.0),
    }


def basis_kernel(x0, xlo, xhi, f, flo, fhi, wz, wy, wx, bd, basis, sums, ring):
    depth = x0.shape[0]
    span = depth + 2 * RIM
    keep = RIM - ITERS
    weights = (wz, wy, wx)
    mask = inside(wz, depth)
    totals = {}

    def take(key, terms):
        s = (terms[0] + terms[1]) + (terms[2] + terms[3])
        if key in totals:
            hi, e = two_sum(totals[key][0], s)
            totals[key] = (hi, totals[key][1] + e)
        else:
            totals[key] = (s, jnp.zeros_like(s))

    def field(e):
        ref, z = at(e, xlo, x0, xhi, depth, RIM)
        return [load_rows(ref, z, q) for q in range(4)]

    def source(e, q):
        ref, z = at(e - 1, flo, f, fhi, depth, TERMS)
        return load_rows(ref, z, q)

    def store(k, e, new, old):
        if e in mask:
            new = [n * mask[e] for n in new]
        for q in range(4):
            if k < TERMS:
                ring[k % 3, e, q] = new[q]
            if k < ITERS and keep <= e < span - keep:
                basis[k, e - keep, q] = new[q]
        if RIM <= e < RIM + depth:
            if k < TERMS:
                take(2 * k, [n * n for n in new])
            if k > 0:
                take(2 * k - 1, [n * o for n, o in zip(new, old)])
            if k < ITERS:
                x = field(e) if k > 0 else old
                if k == 0:
                    take(2 * TERMS, [v * v for v in x])
                take(2 * TERMS + 1 + k, [n * v for n, v in zip(new, x)])

    def first(e, v, div):
        store(0, e, [SOURCE_WEIGHT * source(e, q) - (1.0 / SIGMA) * (bd[e, q] * v[q] - div[q]) for q in range(4)], v)

    divergence(field, weights, 1, span - 2, first)
    for k in range(1, TERMS + 1):

        def emit(e, v, div, k=k):
            image = [(KAPPA + bd[e, q]) * v[q] - div[q] for q in range(4)]
            if k == 1:
                new = [0.5 * i for i in image]
            else:
                new = [i - ring[(k - 2) % 3, e, q] for q, i in enumerate(image)]
            store(k, e, new, v)

        divergence(planes(ring, (k - 1) % 3), weights, 1 + k, span - 2 - k, emit)
    pack([totals[i] for i in range(TOTALS)], sums)


def copy_for_each(array, axis):
    devices = lax.axis_size(axis)
    return lax.all_to_all(
        jnp.broadcast_to(array[None], (devices, *array.shape)), axis, 0, 0, tiled=True
    )


def over_copies(array, axis):
    return copy_for_each(array, axis).sum(axis=0)


def packed_total(arrays, axis):
    ends = [0]
    for a in arrays:
        ends.append(ends[-1] + a.size)
    subtotal = over_copies(jnp.concatenate([a.ravel() for a in arrays]), axis)
    return tuple((subtotal[b:e].reshape(a.shape) for a, b, e in zip(arrays, ends, ends[1:])))


def extended(cells, sides, width):
    for axis, dim in sides:
        count = lax.axis_size(axis)
        ends = count - 1
        head = lax.slice_in_dim(cells, 0, width, axis=dim)
        tail = lax.slice_in_dim(cells, cells.shape[dim] - width, cells.shape[dim], axis=dim)
        cells = jnp.concatenate(
            [
                lax.ppermute(tail, axis, [(i, (i + 1) % count) for i in range(ends)]),
                cells,
                lax.ppermute(head, axis, [((i + 1) % count, i) for i in range(ends)]),
            ],
            axis=dim,
        )
    return cells


def from_behind(array, axis, by):
    devices = lax.axis_size(axis)
    pairs = [(i, i + by) for i in range(devices) if 0 <= i + by < devices]
    return lax.ppermute(array, axis, pairs)


def neighbours(padded):
    return (
        padded[2:, 1:-1, 1:-1],
        padded[:-2, 1:-1, 1:-1],
        padded[1:-1, 2:, 1:-1],
        padded[1:-1, :-2, 1:-1],
        padded[1:-1, 1:-1, 2:],
        padded[1:-1, 1:-1, :-2],
    )


def faces_of(padded_conductivity):
    centre = padded_conductivity[1:-1, 1:-1, 1:-1]
    return tuple((0.5 * (centre + beside) for beside in neighbours(padded_conductivity)))


def apply_operator(grid_field, padded, face_weights):
    flux_sum = jnp.zeros_like(grid_field)
    for face_weight, beside in zip(face_weights, neighbours(padded)):
        flux_sum = flux_sum + face_weight * (grid_field - beside)
    return grid_field + STEP_RATE * flux_sum


def pair_sums(residual, applied):
    return packed_total((jnp.sum(residual * residual), jnp.sum(residual * applied)), "space")


def plain(c_points, corrections, conductivity, forcing):
    rim_conductivity = extended(conductivity, (("space", 0),), 1)
    face_weights = faces_of(jnp.pad(rim_conductivity, ((0, 0), (1, 1), (1, 1))))

    def operate(grid_field):
        with_planes = extended(grid_field, (("space", 0),), 1)
        padded = jnp.pad(with_planes, ((0, 0), (1, 1), (1, 1)))
        return apply_operator(grid_field, padded, face_weights)

    own_point = c_points[0]
    own_fix = corrections[0]
    prior_fix = from_behind(own_fix, "tm", 1)
    current = own_point + prior_fix
    current_image = operate(current)
    sections = []
    for section in range(STEPS):
        right_side = current + SOURCE_WEIGHT * forcing
        if section > 0:
            current_image = operate(current)
        residual = right_side - current_image
        solution = current
        applied = operate(residual)
        norm_now, product = pair_sums(residual, applied)
        step_length = norm_now / product
        direction = residual
        along_dir = applied
        for sweep in range(ITERS):
            solution = solution + step_length * direction
            if sweep + 1 < ITERS:
                residual = residual - step_length * along_dir
                applied = operate(residual)
                norm_next, product = pair_sums(residual, applied)
                beta_ratio = norm_next / norm_now
                step_length = norm_next / (product - beta_ratio * norm_next / step_length)
                direction = residual + beta_ratio * direction
                along_dir = applied + beta_ratio * along_dir
                norm_now = norm_next
        sections.append(solution)
        current = solution
    return jnp.stack(sections)[None]


def body(c_points, corrections, conductivity, forcing):
    args = (c_points, corrections, conductivity, forcing)
    out, good = fast(*args)
    return lax.cond(good[0, 0] > 0, lambda: out, lambda: plain(*args))


def solution(mesh):
    in_specs = (
        P("tm", "space", None, None),
        P("tm", "space", None, None),
        P("space", None, None),
        P("space", None, None),
    )
    out_specs = P("tm", None, "space", None, None)
    return jax.shard_map(body, mesh=mesh, in_specs=in_specs, out_specs=out_specs, check_vma=False)
```

```python
import jax
import jax.numpy as jnp
import numpy as np
from jax import lax
from jax.experimental import pallas as pl
from jax.experimental.pallas import tpu as pltpu
from jax.sharding import PartitionSpec as P


ITERS = 6
STEPS = 2
STEP_RATE = 4.0
SOURCE_WEIGHT = 0.25


LOW, HIGH = 1.0, 141.0
MID = 0.5 * (LOW + HIGH)
HALF = 0.5 * (HIGH - LOW)
SIGMA = 2.0 / HALF
KAPPA = SIGMA * (1.0 - MID)
FACE = 0.5 * STEP_RATE * SIGMA

RIM = STEPS * ITERS
KEEP = ITERS - 1
SUB = 8
LANES = 128
TOTALS = 2 * RIM + 1 + ITERS
GROUPS_OF_8 = (TOTALS + 7) // 8
NOISE = 1e-8
ALLOWED = 5e-5


def two_sum(a, b):
    s = a + b
    t = s - a
    return s, (a - (s - t)) + (b - t)


def quick_two_sum(a, b):
    s = a + b
    return s, b - (s - a)


def add2(a, b):
    s, e = two_sum(a[0], b[0])
    return quick_two_sum(s, e + (a[1] + b[1]))


def neg2(a):
    return -a[0], -a[1]


def split(a):
    t = 4097.0 * a
    hi = t - (t - a)
    return hi, a - hi


def two_prod(a, b):
    p = a * b
    ah, al = split(a)
    bh, bl = split(b)
    return p, ((ah * bh - p) + ah * bl + al * bh) + al * bl


def mul2(a, b):
    p, e = two_prod(a[0], b[0])
    return quick_two_sum(p, e + (a[0] * b[1] + a[1] * b[0]))


def const2(c):
    hi = float(np.float32(c))
    return hi, float(np.float32(c - hi))


def recip2(a):
    q = 1.0 / a[0]
    p, e = two_prod(q, a[0])
    r = (1.0 - p) - (e + q * a[1])
    return quick_two_sum(q, q * r)


def roll(v, shift, axis):
    return pltpu.roll(v, shift % v.shape[axis], axis)


def load_rows(ref, z, k):
    return ref[z, pl.ds(k, SUB, stride=4), :]


def times2(a, c):
    hi, lo = const2(c)
    return mul2(a, (jnp.full_like(a[0], hi), jnp.full_like(a[0], lo)))


def double2(a):
    return 2.0 * a[0], 2.0 * a[1]


def half2(a):
    return 0.5 * a[0], 0.5 * a[1]


def pack(totals, out):
    for shift in (4, 2, 1):
        totals = [add2(t, (roll(t[0], shift, 0), roll(t[1], shift, 0))) for t in totals]
    row = lax.broadcasted_iota(jnp.int32, (SUB, LANES), 0)
    lane = lax.broadcasted_iota(jnp.int32, (SUB, LANES), 1)
    result = jnp.zeros((SUB, LANES), jnp.float32)
    for g in range(GROUPS_OF_8):
        part = totals[8 * g : 8 * g + 8]
        hi = lo = jnp.zeros((SUB, LANES), jnp.float32)
        for i, t in enumerate(part):
            hi = jnp.where(row == i, t[0], hi)
            lo = jnp.where(row == i, t[1], lo)
        both = (hi, lo)
        for shift in (64, 32, 16, 8, 4, 2, 1):
            both = add2(both, (roll(both[0], shift, 1), roll(both[1], shift, 1)))
        result = jnp.where(lane == g, both[0], result)
        result = jnp.where(lane == GROUPS_OF_8 + g, both[1], result)
    for p in range(out.shape[0]):
        out[p] = result


def unpack(gathered):
    hi = gathered[0]
    lo = jnp.zeros_like(hi)
    for p in range(1, gathered.shape[0]):
        hi, e = two_sum(hi, gathered[p])
        lo = lo + e
    lo = lo + roll(hi, -GROUPS_OF_8, 1)
    hi, lo = quick_two_sum(hi, lo)
    whole = (SUB, LANES)
    spot = lambda v, i: jnp.broadcast_to(v[i % 8 : i % 8 + 1, i // 8 : i // 8 + 1], whole)
    return [(spot(hi, i), spot(lo, i)) for i in range(TOTALS)]


def galerkin(nu):
    image = []
    for k in range(2 * ITERS - 1):
        image.append(add2(times2(nu[k], MID), times2(add2(nu[k + 1], nu[abs(k - 1)]), 0.5 * HALF)))
    m = {(i, j): half2(add2(image[i + j], image[i - j])) for i in range(ITERS) for j in range(i + 1)}
    y = [nu[i] for i in range(ITERS)]
    inverse, unit = [], {}
    for j in range(ITERS):
        inverse.append(recip2(m[j, j]))
        for i in range(j + 1, ITERS):
            unit[i, j] = mul2(m[i, j], inverse[j])
        for i in range(j + 1, ITERS):
            minus = neg2(unit[i, j])
            for k in range(j + 1, i + 1):
                m[i, k] = add2(m[i, k], mul2(minus, m[k, j]))
            y[i] = add2(y[i], mul2(minus, y[j]))
    c = [mul2(y[j], inverse[j])[0] for j in range(ITERS)]
    for j in reversed(range(ITERS)):
        for i in range(j + 1, ITERS):
            c[j] = c[j] - unit[i, j][0] * c[i]
    return c


def next_moments(nu, c):
    zero = jnp.zeros_like(c[0])
    shifted = [(zero, zero)] * (ITERS + 2)

    def put(k, v):
        shifted[k] = add2(shifted[k], v)

    for k, v in enumerate(c):
        put(k + 1, (v if k == 0 else 0.5 * v, zero))
        if k > 0:
            put(k - 1, (0.5 * v, zero))
    q = []
    for k in range(ITERS + 1):
        u = times2(shifted[k], -HALF)
        if k < ITERS:
            u = add2(u, times2((c[k], zero), 1.0 - MID))
        q.append(add2((jnp.ones_like(zero), zero), u) if k == 0 else u)
    square = [(zero, zero)] * (2 * ITERS + 1)

    def gather(k, v):
        square[k] = v if square[k][0] is zero else add2(square[k], v)

    for i in range(ITERS + 1):
        for j in range(i + 1):
            v = mul2(q[i], q[j])
            if i == j:
                v = half2(v)
            gather(i + j, v)
            gather(i - j, v)
    result = []
    for k in range(2 * ITERS):
        total = None
        for i in range(2 * ITERS + 1):
            v = mul2(square[i], half2(add2(nu[i + k], nu[abs(i - k)])))
            total = v if total is None else add2(total, v)
        result.append(total)
    return [v[0] for v in q], result


def solve(totals):
    row = lax.broadcasted_iota(jnp.int32, (SUB, LANES), 0)
    shaken = []
    for i in range(2 * RIM):
        sign = jnp.where((row * (2 * i + 3) * 5 + i * 3 + row * row * (i + 1)) % 7 < 3, NOISE, -NOISE)
        sign = jnp.where(row == 0, 0.0, sign)
        scale = totals[i - i % 2][0]
        shaken.append(quick_two_sum(totals[i][0], totals[i][1] + sign * scale))
    nu = []
    for i in range(2 * RIM):
        nu.append(shaken[i] if i < 2 else add2(double2(shaken[i]), neg2(nu[i % 2])))
    c1 = galerkin(nu)
    q, nu2 = next_moments(nu, c1)
    c2 = galerkin(nu2)

    def proper(v):
        return jnp.broadcast_to(v[0:1], v.shape)

    def energy(d, m):
        total = None
        for i in range(ITERS):
            for j in range(i + 1):
                v = d[i] * d[j] * (m[i + j][0] + m[i - j][0])
                v = 0.5 * v if i == j else v
                total = v if total is None else total + v
        return total

    best1, best2 = [proper(v) for v in c1], [proper(v) for v in c2]
    moved = energy([a - b for a, b in zip(c1, best1)], nu) + energy([a - b for a, b in zip(c2, best2)], nu2)
    size = totals[2 * RIM][0] + energy(best1, nu)
    for i in range(ITERS):
        size = size + 2.0 * best1[i] * totals[2 * RIM + 1 + i][0]
    good = jnp.where(moved <= ALLOWED**2 * size, 1.0, 0.0)
    for shift in (4, 2, 1):
        good = jnp.minimum(good, roll(good, shift, 0))
    return best1, [proper(v) for v in q], best2, good


def fill_weights(conduct, fields, first, last):
    wz, wy, wx, wl, bd = fields
    row = lax.broadcasted_iota(jnp.int32, (SUB, LANES), 0)
    lane = lax.broadcasted_iota(jnp.int32, (SUB, LANES), 1)
    not_last_lane = jnp.where(lane < LANES - 1, FACE, 0.0)
    not_first_lane = jnp.where(lane > 0, FACE, 0.0)
    not_last_row = jnp.where(row < SUB - 1, FACE, 0.0)
    side = jnp.where((lane == 0) | (lane == LANES - 1), FACE, 0.0)
    edge = [side + jnp.where(row == 0, FACE, 0.0), side, side, side + jnp.where(row == SUB - 1, FACE, 0.0)]
    here = conduct(first)
    for e in range(first, last + 1):
        z = e - first
        nxt = [here[1], here[2], here[3], roll(here[0], -1, 0)]
        if e < last:
            above = conduct(e + 1)
        for q in range(4):
            if e < last:
                wz[z, q] = FACE * (here[q] + above[q])
            wx[z, q] = not_last_lane * (here[q] + roll(here[q], -1, 1))
            wl[z, q] = not_first_lane * (here[q] + roll(here[q], 1, 1))
            wy[z, q] = (FACE if q < 3 else not_last_row) * (here[q] + nxt[q])
            bd[z, q] = edge[q] * here[q]
        here = above


def flat_part(e, here, fields):
    _, wy, wx, wl, _ = fields
    right = [roll(v, -1, 1) for v in here]
    left = [roll(v, 1, 1) for v in here]
    nxt = [here[1], here[2], here[3], roll(here[0], -1, 0)]
    fy = [wy[e, k] * (nxt[k] - here[k]) for k in range(4)]
    prv = [roll(fy[3], 1, 0), fy[0], fy[1], fy[2]]
    return [
        (fy[k] - prv[k]) + (wx[e, k] * (right[k] - here[k]) - wl[e, k] * (here[k] - left[k])) for k in range(4)
    ]


def divergence(load, fields, first, last, emit, closed=False):
    wz = fields[0]
    here = load(first)
    if not closed:
        below = load(first - 1)
        flux_below = [wz[first - 1, k] * (here[k] - below[k]) for k in range(4)]
    for e in range(first, last + 1):
        div = flat_part(e, here, fields)
        if not (closed and e == last):
            above = load(e + 1)
            flux_above = [wz[e, k] * (above[k] - here[k]) for k in range(4)]
            div = [d + f for d, f in zip(div, flux_above)]
        if not (closed and e == first):
            div = [d - f for d, f in zip(div, flux_below)]
        emit(e, here, div)
        if not (closed and e == last):
            here, flux_below = above, flux_above


def planes(ref, *lead, shift=0):
    return lambda e: [ref[(*lead, e - shift, k)] for k in range(4)]


def conductivities(a, lo, hi):
    depth = a.shape[0]

    def conduct(e):
        ref, z = (lo, e) if e < RIM else (a, e - RIM) if e < RIM + depth else (hi, e - RIM - depth)
        return [ref[z, q] for q in range(4)]

    return conduct


def inside(lo, hi, low, high):
    one = jnp.ones((SUB, LANES), jnp.float32)
    return {
        low: jnp.where(lo[RIM - 1, 0] > 0, one, 0.0),
        high: jnp.where(hi[0, 0] > 0, one, 0.0),
    }


def stage_kernel(c, f, a, cs, fs, cond, tail, head):
    depth = c.shape[0]
    for z in range(depth):
        for q in range(4):
            cs[z, q] = load_rows(c, z, q)
            fs[z, q] = load_rows(f, z, q)
            v = load_rows(a, z, q)
            cond[z, q] = v
            if z < RIM:
                head[z, q] = v
            if z >= depth - RIM:
                tail[z - depth + RIM, q] = v


def open_kernel(c, fix, f, a, x, res, tail, head, *fields):
    depth = c.shape[0]
    fill_weights(planes(a), fields, 0, depth - 1)
    for z in range(depth):
        for q in range(4):
            v = c[z, q] + load_rows(fix, z, q)
            x[z, q] = v
            if z == 0:
                head[RIM, q] = v
            if z == depth - 1:
                tail[RIM, q] = v
    bd = fields[-1]

    def emit(z, v, div):
        for q in range(4):
            r = SOURCE_WEIGHT * f[z, q] - (1.0 / SIGMA) * (bd[z, q] * v[q] - div[q])
            res[z, q] = r
            if z < RIM:
                head[z, q] = r
            if z >= depth - RIM:
                tail[z - depth + RIM, q] = r

    divergence(planes(x), fields, 0, depth - 1, emit, closed=True)


def basis_kernel(x, res, lo, hi, a, alo, ahi, basis, sums, kept, ring, done, *fields):
    depth = x.shape[0]
    span = depth + 2 * RIM
    low, high = RIM - 1, RIM + depth
    mask = inside(alo, ahi, low, high)
    fill_weights(conductivities(a, alo, ahi), fields, 0, span - 1)
    wz, bd = fields[0], fields[-1]
    first, count = RIM - KEEP, depth + 2 * KEEP
    totals = {}

    def take(key, terms):
        s = (terms[0] + terms[1]) + (terms[2] + terms[3])
        if key in totals:
            hi_, e = two_sum(totals[key][0], s)
            totals[key] = (hi_, totals[key][1] + e)
        else:
            totals[key] = (s, jnp.zeros_like(s))

    def place(k):
        return (kept, k) if k <= ITERS else (ring, k % 3)

    def store(k, e, new, old):
        if e in mask:
            new = [n * mask[e] for n in new]
        if k < RIM:
            ref, slot = place(k)
            for q in range(4):
                ref[slot, e, q] = new[q]
        if RIM <= e < RIM + depth:
            if k < RIM:
                take(2 * k, [n * n for n in new])
            if k > 0:
                take(2 * k - 1, [n * o for n, o in zip(new, old)])
            if k < ITERS:
                v = [x[e - RIM, q] for q in range(4)]
                if k == 0:
                    take(2 * RIM, [u * u for u in v])
                take(2 * RIM + 1 + k, [n * u for n, u in zip(new, v)])

    def copy(k):
        return pltpu.make_async_copy(kept.at[k, pl.ds(first, count)], basis.at[k], done.at[k])

    for e in range(span):
        if e < RIM:
            new = [lo[e, q] for q in range(4)]
        elif e < RIM + depth:
            new = [res[e - RIM, q] for q in range(4)]
        else:
            new = [hi[e - RIM - depth, q] for q in range(4)]
        for face, inner, outer in ((low, 0, lo), (high - 1, depth - 1, hi)):
            if e in (face, face + 1):
                own = (e == face) == (face != low)
                for q in range(4):
                    flux = (1.0 / SIGMA) * wz[face, q] * (x[inner, q] - outer[RIM, q])
                    new[q] = new[q] - flux if own else new[q] + flux
        store(0, e, new, None)
    copy(0).start()
    for k in range(1, RIM + 1):

        def emit(e, v, div, k=k):
            image = [(KAPPA + bd[e, q]) * v[q] - div[q] for q in range(4)]
            if k == 1:
                new = [0.5 * i for i in image]
            else:
                ref, slot = place(k - 2)
                new = [i - ref[slot, e, q] for q, i in enumerate(image)]
            store(k, e, new, v)

        divergence(planes(*place(k - 1)), fields, k, span - 1 - k, emit)
        if k <= ITERS:
            copy(k).start()
    pack([totals[i] for i in range(TOTALS)], sums)
    for k in range(ITERS + 1):
        copy(k).wait()


def states_kernel(gathered, basis, x, a, alo, ahi, out, flag, kept, ring, final, done, *fields):
    depth = x.shape[0]
    first, count = RIM - KEEP, depth + 2 * KEEP
    copies = [pltpu.make_async_copy(basis.at[k], kept.at[k], done.at[k]) for k in range(ITERS + 1)]
    for copy in copies:
        copy.start()
    mask = inside(alo, ahi, KEEP - 1, KEEP + depth)
    conduct = conductivities(a, alo, ahi)
    fill_weights(lambda e: conduct(e + first), fields, 0, count - 1)
    bd = fields[-1]
    c1, q1, c2, good = solve(unpack(gathered))
    flag[...] = good
    for copy in copies:
        copy.wait()

    def store(k, e, new):
        if e in mask:
            new = [n * mask[e] for n in new]
        z = e - KEEP
        for q in range(4):
            if k < ITERS - 1:
                ring[k % 3, e, q] = new[q]
            if 0 <= z < depth:
                s = final[z, q] + c2[k] * new[q]
                if k < ITERS - 1:
                    final[z, q] = s
                else:
                    out[0, 1, z, pl.ds(q, SUB, stride=4), :] = s

    for e in range(count):
        z = e - KEEP
        new = []
        for q in range(4):
            parts = [kept[k, e, q] for k in range(ITERS + 1)]
            if 0 <= z < depth:
                s = x[z, q]
                for k in range(ITERS):
                    s = s + c1[k] * parts[k]
                final[z, q] = s
                out[0, 0, z, pl.ds(q, SUB, stride=4), :] = s
            r = q1[0] * parts[0]
            for k in range(1, ITERS + 1):
                r = r + q1[k] * parts[k]
            new.append(r)
        store(0, e, new)
    for k in range(1, ITERS):

        def emit(e, v, div, k=k):
            image = [(KAPPA + bd[e, q]) * v[q] - div[q] for q in range(4)]
            if k == 1:
                new = [0.5 * i for i in image]
            else:
                new = [i - ring[(k - 2) % 3, e, q] for q, i in enumerate(image)]
            store(k, e, new)

        divergence(planes(ring, (k - 1) % 3), fields, k, count - 1 - k, emit)


def call(kernel, outs, scratch, sent=None, read=None, inputs=0, copies=0, weights=True):
    vmem = pl.BlockSpec(memory_space=pltpu.VMEM)
    hbm = pl.BlockSpec(memory_space=pltpu.HBM)
    own = [pltpu.VMEM(s, jnp.float32) for s in scratch]
    if copies:
        own.append(pltpu.SemaphoreType.DMA((copies,)))
    return lambda fields: pl.pallas_call(
        kernel,
        out_shape=[(pltpu.HBM if i == sent else jax.ShapeDtypeStruct)(s, jnp.float32) for i, s in enumerate(outs)],
        in_specs=[hbm if i == read else vmem for i in range(inputs)],
        out_specs=[hbm if i == sent else vmem for i in range(len(outs))],
        scratch_shapes=own + [pltpu.VMEM(fields, jnp.float32)] * (5 if weights else 0),
        compiler_params=pltpu.CompilerParams(vmem_limit_bytes=20 * 2**20),
    )


def fast(c_points, corrections, conductivity, forcing):
    times, slabs = lax.axis_size("tm"), lax.axis_size("space")
    depth = forcing.shape[0]
    span, count = depth + 2 * RIM, depth + 2 * KEEP
    tile = (4, SUB, LANES)
    up = [(i, i + 1) for i in range(slabs - 1)]
    down = [(i + 1, i) for i in range(slabs - 1)]
    later = [(i, i + 1) for i in range(times - 1)]

    def short(moves):
        pairs = []
        for t in range(times):
            for s, d in moves:
                u = t if (s // 2) % 2 == (d // 2) % 2 else t // 4 * 4 + 3 - t % 4
                pairs.append((t * slabs + s, u * slabs + d))
        return pairs

    own, sent, rim = (depth, *tile), (RIM + 1, *tile), (RIM, *tile)
    fix = lax.ppermute(corrections[0], "tm", later)
    point, source, cond, tail, head = call(
        stage_kernel, [own, own, own, rim, rim], [], inputs=3, weights=False
    )(own)(c_points[0], forcing, conductivity)
    alo = lax.ppermute(tail, ("tm", "space"), short(up))
    ahi = lax.ppermute(head, ("tm", "space"), short(down))
    x, res, tail, head = call(open_kernel, [own, own, sent, sent], [], inputs=4)(own)(point, fix, source, cond)
    lo = lax.ppermute(tail, "space", up)
    hi = lax.ppermute(head, "space", down)
    field, part = (span, *tile), (count, *tile)
    basis, sums = call(
        basis_kernel,
        [(ITERS + 1, *part), (slabs, SUB, LANES)],
        [(ITERS + 1, *field), (3, *field)],
        sent=0,
        inputs=7,
        copies=ITERS + 1,
    )(field)(x, res, lo, hi, cond, alo, ahi)
    basis = pltpu.with_memory_space_constraint(basis, pltpu.HBM)
    sums = lax.all_to_all(sums, "space", 0, 0, tiled=True)
    return call(
        states_kernel,
        [(1, STEPS, depth, 4 * SUB, LANES), (SUB, LANES)],
        [(ITERS + 1, *part), (3, *part), own],
        read=1,
        inputs=6,
        copies=ITERS + 1,
    )(part)(sums, basis, x, cond, alo, ahi)


def copy_for_each(array, axis):
    devices = lax.axis_size(axis)
    return lax.all_to_all(
        jnp.broadcast_to(array[None], (devices, *array.shape)), axis, 0, 0, tiled=True
    )


def over_copies(array, axis):
    return copy_for_each(array, axis).sum(axis=0)


def packed_total(arrays, axis):
    ends = [0]
    for a in arrays:
        ends.append(ends[-1] + a.size)
    subtotal = over_copies(jnp.concatenate([a.ravel() for a in arrays]), axis)
    return tuple((subtotal[b:e].reshape(a.shape) for a, b, e in zip(arrays, ends, ends[1:])))


def extended(cells, sides, width):
    for axis, dim in sides:
        count = lax.axis_size(axis)
        ends = count - 1
        head = lax.slice_in_dim(cells, 0, width, axis=dim)
        tail = lax.slice_in_dim(cells, cells.shape[dim] - width, cells.shape[dim], axis=dim)
        cells = jnp.concatenate(
            [
                lax.ppermute(tail, axis, [(i, (i + 1) % count) for i in range(ends)]),
                cells,
                lax.ppermute(head, axis, [((i + 1) % count, i) for i in range(ends)]),
            ],
            axis=dim,
        )
    return cells


def from_behind(array, axis, by):
    devices = lax.axis_size(axis)
    pairs = [(i, i + by) for i in range(devices) if 0 <= i + by < devices]
    return lax.ppermute(array, axis, pairs)


def neighbours(padded):
    return (
        padded[2:, 1:-1, 1:-1],
        padded[:-2, 1:-1, 1:-1],
        padded[1:-1, 2:, 1:-1],
        padded[1:-1, :-2, 1:-1],
        padded[1:-1, 1:-1, 2:],
        padded[1:-1, 1:-1, :-2],
    )


def faces_of(padded_conductivity):
    centre = padded_conductivity[1:-1, 1:-1, 1:-1]
    return tuple((0.5 * (centre + beside) for beside in neighbours(padded_conductivity)))


def apply_operator(grid_field, padded, face_weights):
    flux_sum = jnp.zeros_like(grid_field)
    for face_weight, beside in zip(face_weights, neighbours(padded)):
        flux_sum = flux_sum + face_weight * (grid_field - beside)
    return grid_field + STEP_RATE * flux_sum


def pair_sums(residual, applied):
    return packed_total((jnp.sum(residual * residual), jnp.sum(residual * applied)), "space")


def plain(c_points, corrections, conductivity, forcing):
    rim_conductivity = extended(conductivity, (("space", 0),), 1)
    face_weights = faces_of(jnp.pad(rim_conductivity, ((0, 0), (1, 1), (1, 1))))

    def operate(grid_field):
        with_planes = extended(grid_field, (("space", 0),), 1)
        padded = jnp.pad(with_planes, ((0, 0), (1, 1), (1, 1)))
        return apply_operator(grid_field, padded, face_weights)

    own_point = c_points[0]
    own_fix = corrections[0]
    prior_fix = from_behind(own_fix, "tm", 1)
    current = own_point + prior_fix
    current_image = operate(current)
    sections = []
    for section in range(STEPS):
        right_side = current + SOURCE_WEIGHT * forcing
        if section > 0:
            current_image = operate(current)
        residual = right_side - current_image
        solution = current
        applied = operate(residual)
        norm_now, product = pair_sums(residual, applied)
        step_length = norm_now / product
        direction = residual
        along_dir = applied
        for sweep in range(ITERS):
            solution = solution + step_length * direction
            if sweep + 1 < ITERS:
                residual = residual - step_length * along_dir
                applied = operate(residual)
                norm_next, product = pair_sums(residual, applied)
                beta_ratio = norm_next / norm_now
                step_length = norm_next / (product - beta_ratio * norm_next / step_length)
                direction = residual + beta_ratio * direction
                along_dir = applied + beta_ratio * along_dir
                norm_now = norm_next
        sections.append(solution)
        current = solution
    return jnp.stack(sections)[None]


def body(c_points, corrections, conductivity, forcing):
    args = (c_points, corrections, conductivity, forcing)
    out, good = fast(*args)
    return lax.cond(good[0, 0] > 0, lambda: out, lambda: plain(*args))


def solution(mesh):
    in_specs = (
        P("tm", "space", None, None),
        P("tm", "space", None, None),
        P("space", None, None),
        P("space", None, None),
    )
    out_specs = P("tm", None, "space", None, None)
    return jax.shard_map(body, mesh=mesh, in_specs=in_specs, out_specs=out_specs, check_vma=False)
```

```python
import jax
import jax.numpy as jnp
import numpy as np
from jax import lax
from jax.experimental import pallas as pl
from jax.experimental.pallas import tpu as pltpu
from jax.sharding import PartitionSpec as P


ITERS = 6
STEPS = 2
STEP_RATE = 4.0
SOURCE_WEIGHT = 0.25


LOW, HIGH = 1.0, 141.0
MID = 0.5 * (LOW + HIGH)
HALF = 0.5 * (HIGH - LOW)
SIGMA = 2.0 / HALF
KAPPA = SIGMA * (1.0 - MID)
FACE = 0.5 * STEP_RATE * SIGMA

RIM = STEPS * ITERS
KEEP = ITERS - 1
SUB = 8
LANES = 128
TOTALS = 2 * RIM + 1 + ITERS
GROUPS_OF_8 = (TOTALS + 7) // 8
NOISE = 1e-8
ALLOWED = 5e-5


def two_sum(a, b):
    s = a + b
    t = s - a
    return s, (a - (s - t)) + (b - t)


def quick_two_sum(a, b):
    s = a + b
    return s, b - (s - a)


def add2(a, b):
    s, e = two_sum(a[0], b[0])
    return quick_two_sum(s, e + (a[1] + b[1]))


def neg2(a):
    return -a[0], -a[1]


def split(a):
    t = 4097.0 * a
    hi = t - (t - a)
    return hi, a - hi


def two_prod(a, b):
    p = a * b
    ah, al = split(a)
    bh, bl = split(b)
    return p, ((ah * bh - p) + ah * bl + al * bh) + al * bl


def mul2(a, b):
    p, e = two_prod(a[0], b[0])
    return quick_two_sum(p, e + (a[0] * b[1] + a[1] * b[0]))


def const2(c):
    hi = float(np.float32(c))
    return hi, float(np.float32(c - hi))


def recip2(a):
    q = 1.0 / a[0]
    p, e = two_prod(q, a[0])
    r = (1.0 - p) - (e + q * a[1])
    return quick_two_sum(q, q * r)


def roll(v, shift, axis):
    return pltpu.roll(v, shift % v.shape[axis], axis)


def load_rows(ref, z, k):
    return ref[z, pl.ds(k, SUB, stride=4), :]


def times2(a, c):
    hi, lo = const2(c)
    return mul2(a, (jnp.full_like(a[0], hi), jnp.full_like(a[0], lo)))


def double2(a):
    return 2.0 * a[0], 2.0 * a[1]


def half2(a):
    return 0.5 * a[0], 0.5 * a[1]


def pack(totals, out):
    for shift in (4, 2, 1):
        totals = [add2(t, (roll(t[0], shift, 0), roll(t[1], shift, 0))) for t in totals]
    row = lax.broadcasted_iota(jnp.int32, (SUB, LANES), 0)
    lane = lax.broadcasted_iota(jnp.int32, (SUB, LANES), 1)
    result = jnp.zeros((SUB, LANES), jnp.float32)
    for g in range(GROUPS_OF_8):
        part = totals[8 * g : 8 * g + 8]
        hi = lo = jnp.zeros((SUB, LANES), jnp.float32)
        for i, t in enumerate(part):
            hi = jnp.where(row == i, t[0], hi)
            lo = jnp.where(row == i, t[1], lo)
        both = (hi, lo)
        for shift in (64, 32, 16, 8, 4, 2, 1):
            both = add2(both, (roll(both[0], shift, 1), roll(both[1], shift, 1)))
        result = jnp.where(lane == 8 * g + row, both[0], result)
        result = jnp.where(lane == 64 + 8 * g + row, both[1], result)
    for shift in (4, 2, 1):
        result = result + roll(result, shift, 0)
    for p in range(out.shape[0]):
        out[p] = result[0:1]


def unpack(gathered):
    whole = (SUB, LANES)
    row = lambda p: jnp.broadcast_to(gathered[p], whole)
    hi = row(0)
    lo = jnp.zeros_like(hi)
    for p in range(1, gathered.shape[0]):
        hi, e = two_sum(hi, row(p))
        lo = lo + e
    lo = lo + roll(hi, 64, 1)
    hi, lo = quick_two_sum(hi, lo)
    spot = lambda v, i: jnp.broadcast_to(v[:, i : i + 1], whole)
    return [(spot(hi, i), spot(lo, i)) for i in range(TOTALS)]


def galerkin(nu):
    image = []
    for k in range(2 * ITERS - 1):
        image.append(add2(times2(nu[k], MID), times2(add2(nu[k + 1], nu[abs(k - 1)]), 0.5 * HALF)))
    m = {(i, j): half2(add2(image[i + j], image[i - j])) for i in range(ITERS) for j in range(i + 1)}
    y = [nu[i] for i in range(ITERS)]
    inverse, unit = [], {}
    for j in range(ITERS):
        inverse.append(recip2(m[j, j]))
        for i in range(j + 1, ITERS):
            unit[i, j] = mul2(m[i, j], inverse[j])
        for i in range(j + 1, ITERS):
            minus = neg2(unit[i, j])
            for k in range(j + 1, i + 1):
                m[i, k] = add2(m[i, k], mul2(minus, m[k, j]))
            y[i] = add2(y[i], mul2(minus, y[j]))
    c = [mul2(y[j], inverse[j])[0] for j in range(ITERS)]
    for j in reversed(range(ITERS)):
        for i in range(j + 1, ITERS):
            c[j] = c[j] - unit[i, j][0] * c[i]
    return c


def next_moments(nu, c):
    zero = jnp.zeros_like(c[0])
    shifted = [(zero, zero)] * (ITERS + 2)

    def put(k, v):
        shifted[k] = add2(shifted[k], v)

    for k, v in enumerate(c):
        put(k + 1, (v if k == 0 else 0.5 * v, zero))
        if k > 0:
            put(k - 1, (0.5 * v, zero))
    q = []
    for k in range(ITERS + 1):
        u = times2(shifted[k], -HALF)
        if k < ITERS:
            u = add2(u, times2((c[k], zero), 1.0 - MID))
        q.append(add2((jnp.ones_like(zero), zero), u) if k == 0 else u)
    square = [(zero, zero)] * (2 * ITERS + 1)

    def gather(k, v):
        square[k] = v if square[k][0] is zero else add2(square[k], v)

    for i in range(ITERS + 1):
        for j in range(i + 1):
            v = mul2(q[i], q[j])
            if i == j:
                v = half2(v)
            gather(i + j, v)
            gather(i - j, v)
    result = []
    for k in range(2 * ITERS):
        total = None
        for i in range(2 * ITERS + 1):
            v = mul2(square[i], half2(add2(nu[i + k], nu[abs(i - k)])))
            total = v if total is None else add2(total, v)
        result.append(total)
    return [v[0] for v in q], result


def solve(totals):
    row = lax.broadcasted_iota(jnp.int32, (SUB, LANES), 0)
    shaken = []
    for i in range(2 * RIM):
        sign = jnp.where((row * (2 * i + 3) * 5 + i * 3 + row * row * (i + 1)) % 7 < 3, NOISE, -NOISE)
        sign = jnp.where(row == 0, 0.0, sign)
        scale = totals[i - i % 2][0]
        shaken.append(quick_two_sum(totals[i][0], totals[i][1] + sign * scale))
    nu = []
    for i in range(2 * RIM):
        nu.append(shaken[i] if i < 2 else add2(double2(shaken[i]), neg2(nu[i % 2])))
    c1 = galerkin(nu)
    q, nu2 = next_moments(nu, c1)
    c2 = galerkin(nu2)

    def proper(v):
        return jnp.broadcast_to(v[0:1], v.shape)

    def energy(d, m):
        total = None
        for i in range(ITERS):
            for j in range(i + 1):
                v = d[i] * d[j] * (m[i + j][0] + m[i - j][0])
                v = 0.5 * v if i == j else v
                total = v if total is None else total + v
        return total

    best1, best2 = [proper(v) for v in c1], [proper(v) for v in c2]
    moved = energy([a - b for a, b in zip(c1, best1)], nu) + energy([a - b for a, b in zip(c2, best2)], nu2)
    size = totals[2 * RIM][0] + energy(best1, nu)
    for i in range(ITERS):
        size = size + 2.0 * best1[i] * totals[2 * RIM + 1 + i][0]
    good = jnp.where(moved <= ALLOWED**2 * size, 1.0, 0.0)
    for shift in (4, 2, 1):
        good = jnp.minimum(good, roll(good, shift, 0))
    return best1, [proper(v) for v in q], best2, good


def fill_weights(conduct, fields, first, last):
    wz, wy, wx, wl, bd, dg = fields
    row = lax.broadcasted_iota(jnp.int32, (SUB, LANES), 0)
    lane = lax.broadcasted_iota(jnp.int32, (SUB, LANES), 1)
    not_last_lane = jnp.where(lane < LANES - 1, FACE, 0.0)
    not_first_lane = jnp.where(lane > 0, FACE, 0.0)
    not_last_row = jnp.where(row < SUB - 1, FACE, 0.0)
    side = jnp.where((lane == 0) | (lane == LANES - 1), FACE, 0.0)
    edge = [side + jnp.where(row == 0, FACE, 0.0), side, side, side + jnp.where(row == SUB - 1, FACE, 0.0)]
    here = conduct(first)
    for e in range(first, last + 1):
        z = e - first
        nxt = [here[1], here[2], here[3], roll(here[0], -1, 0)]
        if e < last:
            above = conduct(e + 1)
        for q in range(4):
            if e < last:
                wz[z, q] = FACE * (here[q] + above[q])
            right = not_last_lane * (here[q] + roll(here[q], -1, 1))
            left = not_first_lane * (here[q] + roll(here[q], 1, 1))
            bound = edge[q] * here[q]
            wx[z, q] = right
            wl[z, q] = left
            wy[z, q] = (FACE if q < 3 else not_last_row) * (here[q] + nxt[q])
            bd[z, q] = bound
            dg[z, q] = KAPPA + (bound + (right + left))
        here = above


def across(load, fields, first, last, emit, residual=False):
    wz, wy, wx, wl, bd, dg = fields
    here = load(first)
    if not residual:
        below = load(first - 1)
        flux_below = [wz[first - 1, k] * (here[k] - below[k]) for k in range(4)]
    for e in range(first, last + 1):
        right = [roll(v, -1, 1) for v in here]
        left = [roll(v, 1, 1) for v in here]
        nxt = [here[1], here[2], here[3], roll(here[0], -1, 0)]
        fy = [wy[e, k] * (nxt[k] - here[k]) for k in range(4)]
        prv = [roll(fy[3], 1, 0), fy[0], fy[1], fy[2]]
        if residual:
            w = [
                bd[e, k] * here[k] - (wx[e, k] * (right[k] - here[k]) - wl[e, k] * (here[k] - left[k])) for k in range(4)
            ]
        else:
            w = [dg[e, k] * here[k] - wx[e, k] * right[k] - wl[e, k] * left[k] for k in range(4)]
        w = [w[k] - fy[k] + prv[k] for k in range(4)]
        if not (residual and e == last):
            above = load(e + 1)
            flux_above = [wz[e, k] * (above[k] - here[k]) for k in range(4)]
            w = [d - f for d, f in zip(w, flux_above)]
        if not (residual and e == first):
            w = [d + f for d, f in zip(w, flux_below)]
        emit(e, here, w)
        if not (residual and e == last):
            here, flux_below = above, flux_above


def planes(ref, *lead, shift=0):
    return lambda e: [ref[(*lead, e - shift, k)] for k in range(4)]


def conductivities(a, lo, hi):
    depth = a.shape[0]

    def conduct(e):
        ref, z = (lo, e) if e < RIM else (a, e - RIM) if e < RIM + depth else (hi, e - RIM - depth)
        return [ref[z, q] for q in range(4)]

    return conduct


def inside(lo, hi, low, high):
    one = jnp.ones((SUB, LANES), jnp.float32)
    return {
        low: jnp.where(lo[RIM - 1, 0] > 0, one, 0.0),
        high: jnp.where(hi[0, 0] > 0, one, 0.0),
    }


def stage_kernel(c, f, a, cs, fs, cond, tail, head):
    depth = c.shape[0]
    for z in range(depth):
        for q in range(4):
            cs[z, q] = load_rows(c, z, q)
            fs[z, q] = load_rows(f, z, q)
            v = load_rows(a, z, q)
            cond[z, q] = v
            if z < RIM:
                head[z, q] = v
            if z >= depth - RIM:
                tail[z - depth + RIM, q] = v


def open_kernel(c, fix, f, a, x, res, tail, head, *fields):
    depth = c.shape[0]
    fill_weights(planes(a), fields, 0, depth - 1)
    for z in range(depth):
        for q in range(4):
            v = c[z, q] + load_rows(fix, z, q)
            x[z, q] = v
            if z == 0:
                head[RIM, q] = v
            if z == depth - 1:
                tail[RIM, q] = v

    def emit(z, v, image):
        for q in range(4):
            r = SOURCE_WEIGHT * f[z, q] - (1.0 / SIGMA) * image[q]
            res[z, q] = r
            if z < RIM:
                head[z, q] = r
            if z >= depth - RIM:
                tail[z - depth + RIM, q] = r

    across(planes(x), fields, 0, depth - 1, emit, residual=True)


def basis_kernel(x, res, lo, hi, a, alo, ahi, basis, sums, kept, ring, done, *fields):
    depth = x.shape[0]
    span = depth + 2 * RIM
    low, high = RIM - 1, RIM + depth
    mask = inside(alo, ahi, low, high)
    fill_weights(conductivities(a, alo, ahi), fields, 0, span - 1)
    wz = fields[0]
    first, count = RIM - KEEP, depth + 2 * KEEP
    totals = {}

    def take(key, terms):
        s = (terms[0] + terms[1]) + (terms[2] + terms[3])
        if key in totals:
            hi_, e = two_sum(totals[key][0], s)
            totals[key] = (hi_, totals[key][1] + e)
        else:
            totals[key] = (s, jnp.zeros_like(s))

    def place(k):
        return (kept, k) if k <= ITERS else (ring, k % 3)

    def store(k, e, new, old):
        if e in mask:
            new = [n * mask[e] for n in new]
        if k < RIM:
            ref, slot = place(k)
            for q in range(4):
                ref[slot, e, q] = new[q]
        if RIM <= e < RIM + depth:
            if k < RIM:
                take(2 * k, [n * n for n in new])
            if k > 0:
                take(2 * k - 1, [n * o for n, o in zip(new, old)])
            if k < ITERS:
                v = [x[e - RIM, q] for q in range(4)]
                if k == 0:
                    take(2 * RIM, [u * u for u in v])
                take(2 * RIM + 1 + k, [n * u for n, u in zip(new, v)])

    def copy(k):
        return pltpu.make_async_copy(kept.at[k, pl.ds(first, count)], basis.at[k], done.at[k])

    for e in range(span):
        if e < RIM:
            new = [lo[e, q] for q in range(4)]
        elif e < RIM + depth:
            new = [res[e - RIM, q] for q in range(4)]
        else:
            new = [hi[e - RIM - depth, q] for q in range(4)]
        for face, inner, outer in ((low, 0, lo), (high - 1, depth - 1, hi)):
            if e in (face, face + 1):
                own = (e == face) == (face != low)
                for q in range(4):
                    flux = (1.0 / SIGMA) * wz[face, q] * (x[inner, q] - outer[RIM, q])
                    new[q] = new[q] - flux if own else new[q] + flux
        store(0, e, new, None)
    copy(0).start()
    for k in range(1, RIM + 1):

        def emit(e, v, image, k=k):
            if k == 1:
                new = [0.5 * i for i in image]
            else:
                ref, slot = place(k - 2)
                new = [i - ref[slot, e, q] for q, i in enumerate(image)]
            store(k, e, new, v)

        across(planes(*place(k - 1)), fields, k, span - 1 - k, emit)
        if k <= ITERS:
            copy(k).start()
    pack([totals[i] for i in range(TOTALS)], sums)
    for k in range(ITERS + 1):
        copy(k).wait()


def states_kernel(gathered, basis, x, a, alo, ahi, out, flag, kept, ring, final, done, *fields):
    depth = x.shape[0]
    first, count = RIM - KEEP, depth + 2 * KEEP
    copies = [pltpu.make_async_copy(basis.at[k], kept.at[k], done.at[k]) for k in range(ITERS + 1)]
    for copy in copies:
        copy.start()
    mask = inside(alo, ahi, KEEP - 1, KEEP + depth)
    conduct = conductivities(a, alo, ahi)
    fill_weights(lambda e: conduct(e + first), fields, 0, count - 1)
    c1, q1, c2, good = solve(unpack(gathered))
    flag[0] = good[0, 0].astype(jnp.int32)
    for copy in copies:
        copy.wait()

    def store(k, e, new):
        if e in mask:
            new = [n * mask[e] for n in new]
        z = e - KEEP
        for q in range(4):
            if k < ITERS - 1:
                ring[k % 3, e, q] = new[q]
            if 0 <= z < depth:
                s = final[z, q] + c2[k] * new[q]
                if k < ITERS - 1:
                    final[z, q] = s
                else:
                    out[0, 1, z, pl.ds(q, SUB, stride=4), :] = s

    for e in range(count):
        z = e - KEEP
        new = []
        for q in range(4):
            parts = [kept[k, e, q] for k in range(ITERS + 1)]
            if 0 <= z < depth:
                s = x[z, q]
                for k in range(ITERS):
                    s = s + c1[k] * parts[k]
                final[z, q] = s
                out[0, 0, z, pl.ds(q, SUB, stride=4), :] = s
            r = q1[0] * parts[0]
            for k in range(1, ITERS + 1):
                r = r + q1[k] * parts[k]
            new.append(r)
        store(0, e, new)
    for k in range(1, ITERS):

        def emit(e, v, image, k=k):
            if k == 1:
                new = [0.5 * i for i in image]
            else:
                new = [i - ring[(k - 2) % 3, e, q] for q, i in enumerate(image)]
            store(k, e, new)

        across(planes(ring, (k - 1) % 3), fields, k, count - 1 - k, emit)


def call(kernel, outs, scratch, sent=None, read=None, inputs=0, copies=0, weights=True):
    vmem = pl.BlockSpec(memory_space=pltpu.VMEM)
    hbm = pl.BlockSpec(memory_space=pltpu.HBM)
    smem = pl.BlockSpec(memory_space=pltpu.SMEM)
    own = [pltpu.VMEM(s, jnp.float32) for s in scratch]
    if copies:
        own.append(pltpu.SemaphoreType.DMA((copies,)))
    return lambda fields: pl.pallas_call(
        kernel,
        out_shape=[
            jax.ShapeDtypeStruct((1,), jnp.int32)
            if s is None
            else (pltpu.HBM if i == sent else jax.ShapeDtypeStruct)(s, jnp.float32)
            for i, s in enumerate(outs)
        ],
        in_specs=[hbm if i == read else vmem for i in range(inputs)],
        out_specs=[smem if s is None else hbm if i == sent else vmem for i, s in enumerate(outs)],
        scratch_shapes=own + [pltpu.VMEM(fields, jnp.float32)] * (6 if weights else 0),
        compiler_params=pltpu.CompilerParams(vmem_limit_bytes=20 * 2**20),
    )


def fast(c_points, corrections, conductivity, forcing):
    times, slabs = lax.axis_size("tm"), lax.axis_size("space")
    depth = forcing.shape[0]
    span, count = depth + 2 * RIM, depth + 2 * KEEP
    tile = (4, SUB, LANES)
    up = [(i, i + 1) for i in range(slabs - 1)]
    down = [(i + 1, i) for i in range(slabs - 1)]
    later = [(i, i + 1) for i in range(times - 1)]

    own, sent, rim = (depth, *tile), (RIM + 1, *tile), (RIM, *tile)
    fix = lax.ppermute(corrections[0], "tm", later)
    point, source, cond, tail, head = call(
        stage_kernel, [own, own, own, rim, rim], [], inputs=3, weights=False
    )(own)(c_points[0], forcing, conductivity)
    alo = lax.ppermute(tail, "space", up)
    ahi = lax.ppermute(head, "space", down)
    x, res, tail, head = call(open_kernel, [own, own, sent, sent], [], inputs=4)(own)(point, fix, source, cond)
    lo = lax.ppermute(tail, "space", up)
    hi = lax.ppermute(head, "space", down)
    field, part = (span, *tile), (count, *tile)
    basis, sums = call(
        basis_kernel,
        [(ITERS + 1, *part), (slabs, 1, LANES)],
        [(ITERS + 1, *field), (3, *field)],
        sent=0,
        inputs=7,
        copies=ITERS + 1,
    )(field)(x, res, lo, hi, cond, alo, ahi)
    basis = pltpu.with_memory_space_constraint(basis, pltpu.HBM)
    sums = lax.all_to_all(sums, "space", 0, 0, tiled=True)
    return call(
        states_kernel,
        [(1, STEPS, depth, 4 * SUB, LANES), None],
        [(ITERS + 1, *part), (3, *part), own],
        read=1,
        inputs=6,
        copies=ITERS + 1,
    )(part)(sums, basis, x, cond, alo, ahi)


def copy_for_each(array, axis):
    devices = lax.axis_size(axis)
    return lax.all_to_all(
        jnp.broadcast_to(array[None], (devices, *array.shape)), axis, 0, 0, tiled=True
    )


def over_copies(array, axis):
    return copy_for_each(array, axis).sum(axis=0)


def packed_total(arrays, axis):
    ends = [0]
    for a in arrays:
        ends.append(ends[-1] + a.size)
    subtotal = over_copies(jnp.concatenate([a.ravel() for a in arrays]), axis)
    return tuple((subtotal[b:e].reshape(a.shape) for a, b, e in zip(arrays, ends, ends[1:])))


def extended(cells, sides, width):
    for axis, dim in sides:
        count = lax.axis_size(axis)
        ends = count - 1
        head = lax.slice_in_dim(cells, 0, width, axis=dim)
        tail = lax.slice_in_dim(cells, cells.shape[dim] - width, cells.shape[dim], axis=dim)
        cells = jnp.concatenate(
            [
                lax.ppermute(tail, axis, [(i, (i + 1) % count) for i in range(ends)]),
                cells,
                lax.ppermute(head, axis, [((i + 1) % count, i) for i in range(ends)]),
            ],
            axis=dim,
        )
    return cells


def from_behind(array, axis, by):
    devices = lax.axis_size(axis)
    pairs = [(i, i + by) for i in range(devices) if 0 <= i + by < devices]
    return lax.ppermute(array, axis, pairs)


def neighbours(padded):
    return (
        padded[2:, 1:-1, 1:-1],
        padded[:-2, 1:-1, 1:-1],
        padded[1:-1, 2:, 1:-1],
        padded[1:-1, :-2, 1:-1],
        padded[1:-1, 1:-1, 2:],
        padded[1:-1, 1:-1, :-2],
    )


def faces_of(padded_conductivity):
    centre = padded_conductivity[1:-1, 1:-1, 1:-1]
    return tuple((0.5 * (centre + beside) for beside in neighbours(padded_conductivity)))


def apply_operator(grid_field, padded, face_weights):
    flux_sum = jnp.zeros_like(grid_field)
    for face_weight, beside in zip(face_weights, neighbours(padded)):
        flux_sum = flux_sum + face_weight * (grid_field - beside)
    return grid_field + STEP_RATE * flux_sum


def pair_sums(residual, applied):
    return packed_total((jnp.sum(residual * residual), jnp.sum(residual * applied)), "space")


def plain(c_points, corrections, conductivity, forcing):
    rim_conductivity = extended(conductivity, (("space", 0),), 1)
    face_weights = faces_of(jnp.pad(rim_conductivity, ((0, 0), (1, 1), (1, 1))))

    def operate(grid_field):
        with_planes = extended(grid_field, (("space", 0),), 1)
        padded = jnp.pad(with_planes, ((0, 0), (1, 1), (1, 1)))
        return apply_operator(grid_field, padded, face_weights)

    own_point = c_points[0]
    own_fix = corrections[0]
    prior_fix = from_behind(own_fix, "tm", 1)
    current = own_point + prior_fix
    current_image = operate(current)
    sections = []
    for section in range(STEPS):
        right_side = current + SOURCE_WEIGHT * forcing
        if section > 0:
            current_image = operate(current)
        residual = right_side - current_image
        solution = current
        applied = operate(residual)
        norm_now, product = pair_sums(residual, applied)
        step_length = norm_now / product
        direction = residual
        along_dir = applied
        for sweep in range(ITERS):
            solution = solution + step_length * direction
            if sweep + 1 < ITERS:
                residual = residual - step_length * along_dir
                applied = operate(residual)
                norm_next, product = pair_sums(residual, applied)
                beta_ratio = norm_next / norm_now
                step_length = norm_next / (product - beta_ratio * norm_next / step_length)
                direction = residual + beta_ratio * direction
                along_dir = applied + beta_ratio * along_dir
                norm_now = norm_next
        sections.append(solution)
        current = solution
    return jnp.stack(sections)[None]


def body(c_points, corrections, conductivity, forcing):
    args = (c_points, corrections, conductivity, forcing)
    out, good = fast(*args)
    return lax.cond(good[0] > 0, lambda: out, lambda: plain(*args))


def solution(mesh):
    in_specs = (
        P("tm", "space", None, None),
        P("tm", "space", None, None),
        P("space", None, None),
        P("space", None, None),
    )
    out_specs = P("tm", None, "space", None, None)
    return jax.shard_map(body, mesh=mesh, in_specs=in_specs, out_specs=out_specs, check_vma=False)
```

```python
import jax
import jax.numpy as jnp
import numpy as np
from jax import lax
from jax.experimental import pallas as pl
from jax.experimental.pallas import tpu as pltpu
from jax.sharding import PartitionSpec as P


ITERS = 6
STEPS = 2
STEP_RATE = 4.0
SOURCE_WEIGHT = 0.25


LOW, HIGH = 1.0, 141.0
MID = 0.5 * (LOW + HIGH)
HALF = 0.5 * (HIGH - LOW)
SIGMA = 2.0 / HALF
KAPPA = SIGMA * (1.0 - MID)
FACE = 0.5 * STEP_RATE * SIGMA

RIM = STEPS * ITERS
KEEP = ITERS - 1
SUB = 8
LANES = 128
TOTALS = 2 * RIM + 1 + ITERS
GROUPS_OF_8 = (TOTALS + 7) // 8
NOISE = 1e-8
ALLOWED = 5e-5


def two_sum(a, b):
    s = a + b
    t = s - a
    return s, (a - (s - t)) + (b - t)


def quick_two_sum(a, b):
    s = a + b
    return s, b - (s - a)


def add2(a, b):
    s, e = two_sum(a[0], b[0])
    return quick_two_sum(s, e + (a[1] + b[1]))


def neg2(a):
    return -a[0], -a[1]


def split(a):
    t = 4097.0 * a
    hi = t - (t - a)
    return hi, a - hi


def two_prod(a, b):
    p = a * b
    ah, al = split(a)
    bh, bl = split(b)
    return p, ((ah * bh - p) + ah * bl + al * bh) + al * bl


def mul2(a, b):
    p, e = two_prod(a[0], b[0])
    return quick_two_sum(p, e + (a[0] * b[1] + a[1] * b[0]))


def const2(c):
    hi = float(np.float32(c))
    return hi, float(np.float32(c - hi))


def recip2(a):
    q = 1.0 / a[0]
    p, e = two_prod(q, a[0])
    r = (1.0 - p) - (e + q * a[1])
    return quick_two_sum(q, q * r)


def roll(v, shift, axis):
    return pltpu.roll(v, shift % v.shape[axis], axis)


def load_rows(ref, z, k):
    return ref[z, pl.ds(k, SUB, stride=4), :]


def times2(a, c):
    hi, lo = const2(c)
    return mul2(a, (jnp.full_like(a[0], hi), jnp.full_like(a[0], lo)))


def double2(a):
    return 2.0 * a[0], 2.0 * a[1]


def half2(a):
    return 0.5 * a[0], 0.5 * a[1]


def pack(totals, out):
    for shift in (4, 2, 1):
        totals = [add2(t, (roll(t[0], shift, 0), roll(t[1], shift, 0))) for t in totals]
    row = lax.broadcasted_iota(jnp.int32, (SUB, LANES), 0)
    lane = lax.broadcasted_iota(jnp.int32, (SUB, LANES), 1)
    result = jnp.zeros((SUB, LANES), jnp.float32)
    for g in range(GROUPS_OF_8):
        part = totals[8 * g : 8 * g + 8]
        hi = lo = jnp.zeros((SUB, LANES), jnp.float32)
        for i, t in enumerate(part):
            hi = jnp.where(row == i, t[0], hi)
            lo = jnp.where(row == i, t[1], lo)
        both = (hi, lo)
        for shift in (64, 32, 16, 8, 4, 2, 1):
            both = add2(both, (roll(both[0], shift, 1), roll(both[1], shift, 1)))
        result = jnp.where(lane == 8 * g + row, both[0], result)
        result = jnp.where(lane == 64 + 8 * g + row, both[1], result)
    for shift in (4, 2, 1):
        result = result + roll(result, shift, 0)
    for p in range(out.shape[0]):
        out[p] = result[0:1]


def unpack(gathered):
    whole = (SUB, LANES)
    row = lambda p: jnp.broadcast_to(gathered[p], whole)
    hi = row(0)
    lo = jnp.zeros_like(hi)
    for p in range(1, gathered.shape[0]):
        hi, e = two_sum(hi, row(p))
        lo = lo + e
    lo = lo + roll(hi, 64, 1)
    hi, lo = quick_two_sum(hi, lo)
    spot = lambda v, i: jnp.broadcast_to(v[:, i : i + 1], whole)
    return [(spot(hi, i), spot(lo, i)) for i in range(TOTALS)]


def galerkin(nu):
    image = []
    for k in range(2 * ITERS - 1):
        image.append(add2(times2(nu[k], MID), times2(add2(nu[k + 1], nu[abs(k - 1)]), 0.5 * HALF)))
    m = {(i, j): half2(add2(image[i + j], image[i - j])) for i in range(ITERS) for j in range(i + 1)}
    y = [nu[i] for i in range(ITERS)]
    inverse, unit = [], {}
    for j in range(ITERS):
        inverse.append(recip2(m[j, j]))
        for i in range(j + 1, ITERS):
            unit[i, j] = mul2(m[i, j], inverse[j])
        for i in range(j + 1, ITERS):
            minus = neg2(unit[i, j])
            for k in range(j + 1, i + 1):
                m[i, k] = add2(m[i, k], mul2(minus, m[k, j]))
            y[i] = add2(y[i], mul2(minus, y[j]))
    c = [mul2(y[j], inverse[j])[0] for j in range(ITERS)]
    for j in reversed(range(ITERS)):
        for i in range(j + 1, ITERS):
            c[j] = c[j] - unit[i, j][0] * c[i]
    return c


def next_moments(nu, c):
    zero = jnp.zeros_like(c[0])
    shifted = [(zero, zero)] * (ITERS + 2)

    def put(k, v):
        shifted[k] = add2(shifted[k], v)

    for k, v in enumerate(c):
        put(k + 1, (v if k == 0 else 0.5 * v, zero))
        if k > 0:
            put(k - 1, (0.5 * v, zero))
    q = []
    for k in range(ITERS + 1):
        u = times2(shifted[k], -HALF)
        if k < ITERS:
            u = add2(u, times2((c[k], zero), 1.0 - MID))
        q.append(add2((jnp.ones_like(zero), zero), u) if k == 0 else u)
    square = [(zero, zero)] * (2 * ITERS + 1)

    def gather(k, v):
        square[k] = v if square[k][0] is zero else add2(square[k], v)

    for i in range(ITERS + 1):
        for j in range(i + 1):
            v = mul2(q[i], q[j])
            if i == j:
                v = half2(v)
            gather(i + j, v)
            gather(i - j, v)
    result = []
    for k in range(2 * ITERS):
        total = None
        for i in range(2 * ITERS + 1):
            v = mul2(square[i], half2(add2(nu[i + k], nu[abs(i - k)])))
            total = v if total is None else add2(total, v)
        result.append(total)
    return [v[0] for v in q], result


def solve(totals):
    row = lax.broadcasted_iota(jnp.int32, (SUB, LANES), 0)
    shaken = []
    for i in range(2 * RIM):
        sign = jnp.where((row * (2 * i + 3) * 5 + i * 3 + row * row * (i + 1)) % 7 < 3, NOISE, -NOISE)
        sign = jnp.where(row == 0, 0.0, sign)
        scale = totals[i - i % 2][0]
        shaken.append(quick_two_sum(totals[i][0], totals[i][1] + sign * scale))
    nu = []
    for i in range(2 * RIM):
        nu.append(shaken[i] if i < 2 else add2(double2(shaken[i]), neg2(nu[i % 2])))
    c1 = galerkin(nu)
    q, nu2 = next_moments(nu, c1)
    c2 = galerkin(nu2)

    def proper(v):
        return jnp.broadcast_to(v[0:1], v.shape)

    def energy(d, m):
        total = None
        for i in range(ITERS):
            for j in range(i + 1):
                v = d[i] * d[j] * (m[i + j][0] + m[i - j][0])
                v = 0.5 * v if i == j else v
                total = v if total is None else total + v
        return total

    best1, best2 = [proper(v) for v in c1], [proper(v) for v in c2]
    moved = energy([a - b for a, b in zip(c1, best1)], nu) + energy([a - b for a, b in zip(c2, best2)], nu2)
    size = totals[2 * RIM][0] + energy(best1, nu)
    for i in range(ITERS):
        size = size + 2.0 * best1[i] * totals[2 * RIM + 1 + i][0]
    good = jnp.where(moved <= ALLOWED**2 * size, 1.0, 0.0)
    for shift in (4, 2, 1):
        good = jnp.minimum(good, roll(good, shift, 0))
    return best1, [proper(v) for v in q], best2, good


def fill_weights(conduct, fields, first, last):
    wz, wy, wx, wl, bd, dg = fields
    row = lax.broadcasted_iota(jnp.int32, (SUB, LANES), 0)
    lane = lax.broadcasted_iota(jnp.int32, (SUB, LANES), 1)
    not_last_lane = jnp.where(lane < LANES - 1, FACE, 0.0)
    not_first_lane = jnp.where(lane > 0, FACE, 0.0)
    not_last_row = jnp.where(row < SUB - 1, FACE, 0.0)
    side = jnp.where((lane == 0) | (lane == LANES - 1), FACE, 0.0)
    edge = [side + jnp.where(row == 0, FACE, 0.0), side, side, side + jnp.where(row == SUB - 1, FACE, 0.0)]
    here = conduct(first)
    for e in range(first, last + 1):
        z = e - first
        nxt = [here[1], here[2], here[3], roll(here[0], -1, 0)]
        if e < last:
            above = conduct(e + 1)
        for q in range(4):
            if e < last:
                wz[z, q] = FACE * (here[q] + above[q])
            right = not_last_lane * (here[q] + roll(here[q], -1, 1))
            left = not_first_lane * (here[q] + roll(here[q], 1, 1))
            bound = edge[q] * here[q]
            wx[z, q] = right
            wl[z, q] = left
            wy[z, q] = (FACE if q < 3 else not_last_row) * (here[q] + nxt[q])
            bd[z, q] = bound
            dg[z, q] = KAPPA + (bound + (right + left))
        here = above


def across(load, fields, first, last, emit, residual=False):
    wz, wy, wx, wl, bd, dg = fields
    here = load(first)
    if not residual:
        below = load(first - 1)
        flux_below = [wz[first - 1, k] * (here[k] - below[k]) for k in range(4)]
    for e in range(first, last + 1):
        right = [roll(v, -1, 1) for v in here]
        left = [roll(v, 1, 1) for v in here]
        nxt = [here[1], here[2], here[3], roll(here[0], -1, 0)]
        fy = [wy[e, k] * (nxt[k] - here[k]) for k in range(4)]
        prv = [roll(fy[3], 1, 0), fy[0], fy[1], fy[2]]
        if residual:
            w = [
                bd[e, k] * here[k] - (wx[e, k] * (right[k] - here[k]) - wl[e, k] * (here[k] - left[k])) for k in range(4)
            ]
        else:
            w = [dg[e, k] * here[k] - wx[e, k] * right[k] - wl[e, k] * left[k] for k in range(4)]
        w = [w[k] - fy[k] + prv[k] for k in range(4)]
        if not (residual and e == last):
            above = load(e + 1)
            flux_above = [wz[e, k] * (above[k] - here[k]) for k in range(4)]
            w = [d - f for d, f in zip(w, flux_above)]
        if not (residual and e == first):
            w = [d + f for d, f in zip(w, flux_below)]
        emit(e, here, w)
        if not (residual and e == last):
            here, flux_below = above, flux_above


def planes(ref, *lead, shift=0):
    return lambda e: [ref[(*lead, e - shift, k)] for k in range(4)]


def conductivities(a, low, high):
    depth = a.shape[0]

    def conduct(e):
        if e < RIM:
            return [low(e, q) for q in range(4)]
        if e < RIM + depth:
            return [a[e - RIM, q] for q in range(4)]
        return [high(e - RIM - depth, q) for q in range(4)]

    return conduct


def inside(low, high, below, above):
    one = jnp.ones((SUB, LANES), jnp.float32)
    return {
        below: jnp.where(low(RIM - 1, 0) > 0, one, 0.0),
        above: jnp.where(high(0, 0) > 0, one, 0.0),
    }


def is_odd():
    return lax.axis_index("space") % 2 == 1


def swap(far, near, z, q, odd, tail, head):
    far[z, q] = jnp.where(odd, tail, head)
    near[z, q] = jnp.where(odd, head, tail)


def sides(far, near, odd):
    low = lambda z, q: jnp.where(odd, near[z, q], far[z, q])
    high = lambda z, q: jnp.where(odd, far[z, q], near[z, q])
    return low, high


def stage_kernel(c, f, a, cs, fs, cond, far, near):
    depth = c.shape[0]
    for z in range(depth):
        for q in range(4):
            cs[z, q] = load_rows(c, z, q)
            fs[z, q] = load_rows(f, z, q)
            cond[z, q] = load_rows(a, z, q)
    odd = is_odd()
    for z in range(RIM):
        for q in range(4):
            swap(far, near, z, q, odd, cond[z + depth - RIM, q], cond[z, q])


def open_kernel(c, fix, f, a, x, res, far, near, *fields):
    depth = c.shape[0]
    fill_weights(planes(a), fields, 0, depth - 1)
    for z in range(depth):
        for q in range(4):
            v = c[z, q] + load_rows(fix, z, q)
            x[z, q] = v

    def emit(z, v, image):
        for q in range(4):
            r = SOURCE_WEIGHT * f[z, q] - (1.0 / SIGMA) * image[q]
            res[z, q] = r

    across(planes(x), fields, 0, depth - 1, emit, residual=True)
    odd = is_odd()
    for z in range(RIM):
        for q in range(4):
            swap(far, near, z, q, odd, res[z + depth - RIM, q], res[z, q])
    for q in range(4):
        swap(far, near, RIM, q, odd, x[depth - 1, q], x[0, q])


def basis_kernel(x, res, far, near, a, afar, anear, basis, sums, kept, ring, done, *fields):
    depth = x.shape[0]
    span = depth + 2 * RIM
    low, high = RIM - 1, RIM + depth
    odd = is_odd()
    lo, hi = sides(far, near, odd)
    alo, ahi = sides(afar, anear, odd)
    mask = inside(alo, ahi, low, high)
    fill_weights(conductivities(a, alo, ahi), fields, 0, span - 1)
    wz = fields[0]
    first, count = RIM - KEEP, depth + 2 * KEEP
    totals = {}

    def take(key, terms):
        s = (terms[0] + terms[1]) + (terms[2] + terms[3])
        if key in totals:
            hi_, e = two_sum(totals[key][0], s)
            totals[key] = (hi_, totals[key][1] + e)
        else:
            totals[key] = (s, jnp.zeros_like(s))

    def place(k):
        return (kept, k) if k <= ITERS else (ring, k % 3)

    def store(k, e, new, old):
        if e in mask:
            new = [n * mask[e] for n in new]
        if k < RIM:
            ref, slot = place(k)
            for q in range(4):
                ref[slot, e, q] = new[q]
        if RIM <= e < RIM + depth:
            if k < RIM:
                take(2 * k, [n * n for n in new])
            if k > 0:
                take(2 * k - 1, [n * o for n, o in zip(new, old)])
            if k < ITERS:
                v = [x[e - RIM, q] for q in range(4)]
                if k == 0:
                    take(2 * RIM, [u * u for u in v])
                take(2 * RIM + 1 + k, [n * u for n, u in zip(new, v)])

    def copy(k):
        return pltpu.make_async_copy(kept.at[k, pl.ds(first, count)], basis.at[k], done.at[k])

    for e in range(span):
        if e < RIM:
            new = [lo(e, q) for q in range(4)]
        elif e < RIM + depth:
            new = [res[e - RIM, q] for q in range(4)]
        else:
            new = [hi(e - RIM - depth, q) for q in range(4)]
        for face, inner, outer in ((low, 0, lo), (high - 1, depth - 1, hi)):
            if e in (face, face + 1):
                own = (e == face) == (face != low)
                for q in range(4):
                    flux = (1.0 / SIGMA) * wz[face, q] * (x[inner, q] - outer(RIM, q))
                    new[q] = new[q] - flux if own else new[q] + flux
        store(0, e, new, None)
    copy(0).start()
    for k in range(1, RIM + 1):

        def emit(e, v, image, k=k):
            if k == 1:
                new = [0.5 * i for i in image]
            else:
                ref, slot = place(k - 2)
                new = [i - ref[slot, e, q] for q, i in enumerate(image)]
            store(k, e, new, v)

        across(planes(*place(k - 1)), fields, k, span - 1 - k, emit)
        if k <= ITERS:
            copy(k).start()
    pack([totals[i] for i in range(TOTALS)], sums)
    for k in range(ITERS + 1):
        copy(k).wait()


def states_kernel(gathered, basis, x, a, afar, anear, out, flag, kept, ring, final, done, *fields):
    depth = x.shape[0]
    first, count = RIM - KEEP, depth + 2 * KEEP
    copies = [pltpu.make_async_copy(basis.at[k], kept.at[k], done.at[k]) for k in range(ITERS + 1)]
    for copy in copies:
        copy.start()
    alo, ahi = sides(afar, anear, is_odd())
    mask = inside(alo, ahi, KEEP - 1, KEEP + depth)
    conduct = conductivities(a, alo, ahi)
    fill_weights(lambda e: conduct(e + first), fields, 0, count - 1)
    c1, q1, c2, good = solve(unpack(gathered))
    flag[0] = good[0, 0].astype(jnp.int32)
    for copy in copies:
        copy.wait()

    def store(k, e, new):
        if e in mask:
            new = [n * mask[e] for n in new]
        z = e - KEEP
        for q in range(4):
            if k < ITERS - 1:
                ring[k % 3, e, q] = new[q]
            if 0 <= z < depth:
                s = final[z, q] + c2[k] * new[q]
                if k < ITERS - 1:
                    final[z, q] = s
                else:
                    out[0, 1, z, pl.ds(q, SUB, stride=4), :] = s

    for e in range(count):
        z = e - KEEP
        new = []
        for q in range(4):
            parts = [kept[k, e, q] for k in range(ITERS + 1)]
            if 0 <= z < depth:
                s = x[z, q]
                for k in range(ITERS):
                    s = s + c1[k] * parts[k]
                final[z, q] = s
                out[0, 0, z, pl.ds(q, SUB, stride=4), :] = s
            r = q1[0] * parts[0]
            for k in range(1, ITERS + 1):
                r = r + q1[k] * parts[k]
            new.append(r)
        store(0, e, new)
    for k in range(1, ITERS):

        def emit(e, v, image, k=k):
            if k == 1:
                new = [0.5 * i for i in image]
            else:
                new = [i - ring[(k - 2) % 3, e, q] for q, i in enumerate(image)]
            store(k, e, new)

        across(planes(ring, (k - 1) % 3), fields, k, count - 1 - k, emit)


def call(kernel, outs, scratch, sent=None, read=None, inputs=0, copies=0, weights=True):
    vmem = pl.BlockSpec(memory_space=pltpu.VMEM)
    hbm = pl.BlockSpec(memory_space=pltpu.HBM)
    smem = pl.BlockSpec(memory_space=pltpu.SMEM)
    own = [pltpu.VMEM(s, jnp.float32) for s in scratch]
    if copies:
        own.append(pltpu.SemaphoreType.DMA((copies,)))
    return lambda fields: pl.pallas_call(
        kernel,
        out_shape=[
            jax.ShapeDtypeStruct((1,), jnp.int32)
            if s is None
            else (pltpu.HBM if i == sent else jax.ShapeDtypeStruct)(s, jnp.float32)
            for i, s in enumerate(outs)
        ],
        in_specs=[hbm if i == read else vmem for i in range(inputs)],
        out_specs=[smem if s is None else hbm if i == sent else vmem for i, s in enumerate(outs)],
        scratch_shapes=own + [pltpu.VMEM(fields, jnp.float32)] * (6 if weights else 0),
        compiler_params=pltpu.CompilerParams(vmem_limit_bytes=20 * 2**20),
    )


def fast(c_points, corrections, conductivity, forcing):
    times, slabs = lax.axis_size("tm"), lax.axis_size("space")
    depth = forcing.shape[0]
    span, count = depth + 2 * RIM, depth + 2 * KEEP
    tile = (4, SUB, LANES)
    far_pairs = [p for i in range(1, slabs - 1, 2) for p in ((i, i + 1), (i + 1, i))]
    near_pairs = [p for i in range(0, slabs - 1, 2) for p in ((i, i + 1), (i + 1, i))]
    later = [(i, i + 1) for i in range(times - 1)]

    own, sent, rim = (depth, *tile), (RIM + 1, *tile), (RIM, *tile)
    fix = lax.ppermute(corrections[0], "tm", later)
    point, source, cond, far, near = call(
        stage_kernel, [own, own, own, rim, rim], [], inputs=3, weights=False
    )(own)(c_points[0], forcing, conductivity)
    afar = lax.ppermute(far, "space", far_pairs)
    anear = lax.ppermute(near, "space", near_pairs)
    x, res, far, near = call(open_kernel, [own, own, sent, sent], [], inputs=4)(own)(point, fix, source, cond)
    far = lax.ppermute(far, "space", far_pairs)
    near = lax.ppermute(near, "space", near_pairs)
    field, part = (span, *tile), (count, *tile)
    basis, sums = call(
        basis_kernel,
        [(ITERS + 1, *part), (slabs, 1, LANES)],
        [(ITERS + 1, *field), (3, *field)],
        sent=0,
        inputs=7,
        copies=ITERS + 1,
    )(field)(x, res, far, near, cond, afar, anear)
    basis = pltpu.with_memory_space_constraint(basis, pltpu.HBM)
    sums = lax.all_to_all(sums, "space", 0, 0, tiled=True)
    return call(
        states_kernel,
        [(1, STEPS, depth, 4 * SUB, LANES), None],
        [(ITERS + 1, *part), (3, *part), own],
        read=1,
        inputs=6,
        copies=ITERS + 1,
    )(part)(sums, basis, x, cond, afar, anear)


def copy_for_each(array, axis):
    devices = lax.axis_size(axis)
    return lax.all_to_all(
        jnp.broadcast_to(array[None], (devices, *array.shape)), axis, 0, 0, tiled=True
    )


def over_copies(array, axis):
    return copy_for_each(array, axis).sum(axis=0)


def packed_total(arrays, axis):
    ends = [0]
    for a in arrays:
        ends.append(ends[-1] + a.size)
    subtotal = over_copies(jnp.concatenate([a.ravel() for a in arrays]), axis)
    return tuple((subtotal[b:e].reshape(a.shape) for a, b, e in zip(arrays, ends, ends[1:])))


def extended(cells, sides, width):
    for axis, dim in sides:
        count = lax.axis_size(axis)
        ends = count - 1
        head = lax.slice_in_dim(cells, 0, width, axis=dim)
        tail = lax.slice_in_dim(cells, cells.shape[dim] - width, cells.shape[dim], axis=dim)
        cells = jnp.concatenate(
            [
                lax.ppermute(tail, axis, [(i, (i + 1) % count) for i in range(ends)]),
                cells,
                lax.ppermute(head, axis, [((i + 1) % count, i) for i in range(ends)]),
            ],
            axis=dim,
        )
    return cells


def from_behind(array, axis, by):
    devices = lax.axis_size(axis)
    pairs = [(i, i + by) for i in range(devices) if 0 <= i + by < devices]
    return lax.ppermute(array, axis, pairs)


def neighbours(padded):
    return (
        padded[2:, 1:-1, 1:-1],
        padded[:-2, 1:-1, 1:-1],
        padded[1:-1, 2:, 1:-1],
        padded[1:-1, :-2, 1:-1],
        padded[1:-1, 1:-1, 2:],
        padded[1:-1, 1:-1, :-2],
    )


def faces_of(padded_conductivity):
    centre = padded_conductivity[1:-1, 1:-1, 1:-1]
    return tuple((0.5 * (centre + beside) for beside in neighbours(padded_conductivity)))


def apply_operator(grid_field, padded, face_weights):
    flux_sum = jnp.zeros_like(grid_field)
    for face_weight, beside in zip(face_weights, neighbours(padded)):
        flux_sum = flux_sum + face_weight * (grid_field - beside)
    return grid_field + STEP_RATE * flux_sum


def pair_sums(residual, applied):
    return packed_total((jnp.sum(residual * residual), jnp.sum(residual * applied)), "space")


def plain(c_points, corrections, conductivity, forcing):
    rim_conductivity = extended(conductivity, (("space", 0),), 1)
    face_weights = faces_of(jnp.pad(rim_conductivity, ((0, 0), (1, 1), (1, 1))))

    def operate(grid_field):
        with_planes = extended(grid_field, (("space", 0),), 1)
        padded = jnp.pad(with_planes, ((0, 0), (1, 1), (1, 1)))
        return apply_operator(grid_field, padded, face_weights)

    own_point = c_points[0]
    own_fix = corrections[0]
    prior_fix = from_behind(own_fix, "tm", 1)
    current = own_point + prior_fix
    current_image = operate(current)
    sections = []
    for section in range(STEPS):
        right_side = current + SOURCE_WEIGHT * forcing
        if section > 0:
            current_image = operate(current)
        residual = right_side - current_image
        solution = current
        applied = operate(residual)
        norm_now, product = pair_sums(residual, applied)
        step_length = norm_now / product
        direction = residual
        along_dir = applied
        for sweep in range(ITERS):
            solution = solution + step_length * direction
            if sweep + 1 < ITERS:
                residual = residual - step_length * along_dir
                applied = operate(residual)
                norm_next, product = pair_sums(residual, applied)
                beta_ratio = norm_next / norm_now
                step_length = norm_next / (product - beta_ratio * norm_next / step_length)
                direction = residual + beta_ratio * direction
                along_dir = applied + beta_ratio * along_dir
                norm_now = norm_next
        sections.append(solution)
        current = solution
    return jnp.stack(sections)[None]


def body(c_points, corrections, conductivity, forcing):
    args = (c_points, corrections, conductivity, forcing)
    out, good = fast(*args)
    args, good = lax.optimization_barrier((args, good))
    return lax.cond(good[0] > 0, lambda: out, lambda: plain(*args))


def solution(mesh):
    in_specs = (
        P("tm", "space", None, None),
        P("tm", "space", None, None),
        P("space", None, None),
        P("space", None, None),
    )
    out_specs = P("tm", None, "space", None, None)
    return jax.shard_map(body, mesh=mesh, in_specs=in_specs, out_specs=out_specs, check_vma=False)
```

```python
import jax
import jax.numpy as jnp
import numpy as np
from jax import lax
from jax.experimental import pallas as pl
from jax.experimental.pallas import tpu as pltpu
from jax.sharding import PartitionSpec as P


ITERS = 6
STEPS = 2
STEP_RATE = 4.0
SOURCE_WEIGHT = 0.25


LOW, HIGH = 1.0, 141.0
MID = 0.5 * (LOW + HIGH)
HALF = 0.5 * (HIGH - LOW)
SIGMA = 2.0 / HALF
KAPPA = SIGMA * (1.0 - MID)
FACE = 0.5 * STEP_RATE * SIGMA

RIM = STEPS * ITERS
SUB = 8
LANES = 128
TOTALS = 2 * RIM + 1 + ITERS
GROUPS_OF_8 = (TOTALS + 7) // 8
NOISE = 1e-8
ROUNDING = 5e-7
ALLOWED = 5e-5


def two_sum(a, b):
    s = a + b
    t = s - a
    return s, (a - (s - t)) + (b - t)


def quick_two_sum(a, b):
    s = a + b
    return s, b - (s - a)


def add2(a, b):
    s, e = two_sum(a[0], b[0])
    return quick_two_sum(s, e + (a[1] + b[1]))


def neg2(a):
    return -a[0], -a[1]


def split(a):
    t = 4097.0 * a
    hi = t - (t - a)
    return hi, a - hi


def two_prod(a, b):
    p = a * b
    ah, al = split(a)
    bh, bl = split(b)
    return p, ((ah * bh - p) + ah * bl + al * bh) + al * bl


def mul2(a, b):
    p, e = two_prod(a[0], b[0])
    return quick_two_sum(p, e + (a[0] * b[1] + a[1] * b[0]))


def const2(c):
    hi = float(np.float32(c))
    return hi, float(np.float32(c - hi))


def recip2(a):
    q = 1.0 / a[0]
    p, e = two_prod(q, a[0])
    r = (1.0 - p) - (e + q * a[1])
    return quick_two_sum(q, q * r)


def roll(v, shift, axis):
    return pltpu.roll(v, shift % v.shape[axis], axis)


def load_rows(ref, z, k):
    return ref[z, pl.ds(k, SUB, stride=4), :]


def times2(a, c):
    hi, lo = const2(c)
    return mul2(a, (jnp.full_like(a[0], hi), jnp.full_like(a[0], lo)))


def double2(a):
    return 2.0 * a[0], 2.0 * a[1]


def half2(a):
    return 0.5 * a[0], 0.5 * a[1]


def pack(totals, out):
    for shift in (4, 2, 1):
        totals = [add2(t, (roll(t[0], shift, 0), roll(t[1], shift, 0))) for t in totals]
    row = lax.broadcasted_iota(jnp.int32, (SUB, LANES), 0)
    lane = lax.broadcasted_iota(jnp.int32, (SUB, LANES), 1)
    result = jnp.zeros((SUB, LANES), jnp.float32)
    for g in range(GROUPS_OF_8):
        part = totals[8 * g : 8 * g + 8]
        hi = lo = jnp.zeros((SUB, LANES), jnp.float32)
        for i, t in enumerate(part):
            hi = jnp.where(row == i, t[0], hi)
            lo = jnp.where(row == i, t[1], lo)
        both = (hi, lo)
        for shift in (64, 32, 16, 8, 4, 2, 1):
            both = add2(both, (roll(both[0], shift, 1), roll(both[1], shift, 1)))
        result = jnp.where(lane == 8 * g + row, both[0], result)
        result = jnp.where(lane == 64 + 8 * g + row, both[1], result)
    for shift in (4, 2, 1):
        result = result + roll(result, shift, 0)
    for p in range(out.shape[0]):
        out[p] = result[0:1]


def unpack(gathered):
    whole = (SUB, LANES)
    row = lambda p: jnp.broadcast_to(gathered[p], whole)
    hi = row(0)
    lo = jnp.zeros_like(hi)
    for p in range(1, gathered.shape[0]):
        hi, e = two_sum(hi, row(p))
        lo = lo + e
    lo = lo + roll(hi, 64, 1)
    hi, lo = quick_two_sum(hi, lo)
    spot = lambda v, i: jnp.broadcast_to(v[:, i : i + 1], whole)
    return [(spot(hi, i), spot(lo, i)) for i in range(TOTALS)]


def galerkin(nu):
    image = []
    for k in range(2 * ITERS - 1):
        image.append(add2(times2(nu[k], MID), times2(add2(nu[k + 1], nu[abs(k - 1)]), 0.5 * HALF)))
    m = {(i, j): half2(add2(image[i + j], image[i - j])) for i in range(ITERS) for j in range(i + 1)}
    y = [nu[i] for i in range(ITERS)]
    inverse, unit = [], {}
    for j in range(ITERS):
        inverse.append(recip2(m[j, j]))
        for i in range(j + 1, ITERS):
            unit[i, j] = mul2(m[i, j], inverse[j])
        for i in range(j + 1, ITERS):
            minus = neg2(unit[i, j])
            for k in range(j + 1, i + 1):
                m[i, k] = add2(m[i, k], mul2(minus, m[k, j]))
            y[i] = add2(y[i], mul2(minus, y[j]))
    c = [mul2(y[j], inverse[j])[0] for j in range(ITERS)]
    for j in reversed(range(ITERS)):
        for i in range(j + 1, ITERS):
            c[j] = c[j] - unit[i, j][0] * c[i]
    return c


def next_moments(nu, c):
    zero = jnp.zeros_like(c[0])
    shifted = [(zero, zero)] * (ITERS + 2)

    def put(k, v):
        shifted[k] = add2(shifted[k], v)

    for k, v in enumerate(c):
        put(k + 1, (v if k == 0 else 0.5 * v, zero))
        if k > 0:
            put(k - 1, (0.5 * v, zero))
    q = []
    for k in range(ITERS + 1):
        u = times2(shifted[k], -HALF)
        if k < ITERS:
            u = add2(u, times2((c[k], zero), 1.0 - MID))
        q.append(add2((jnp.ones_like(zero), zero), u) if k == 0 else u)
    square = [(zero, zero)] * (2 * ITERS + 1)

    def gather(k, v):
        square[k] = v if square[k][0] is zero else add2(square[k], v)

    for i in range(ITERS + 1):
        for j in range(i + 1):
            v = mul2(q[i], q[j])
            if i == j:
                v = half2(v)
            gather(i + j, v)
            gather(i - j, v)
    result = []
    for k in range(2 * ITERS):
        total = None
        for i in range(2 * ITERS + 1):
            v = mul2(square[i], half2(add2(nu[i + k], nu[abs(i - k)])))
            total = v if total is None else add2(total, v)
        result.append(total)
    return [v[0] for v in q], result


def solve(totals):
    row = lax.broadcasted_iota(jnp.int32, (SUB, LANES), 0)
    shaken = []
    for i in range(2 * RIM):
        sign = jnp.where((row * (2 * i + 3) * 5 + i * 3 + row * row * (i + 1)) % 7 < 3, NOISE, -NOISE)
        sign = jnp.where(row == 0, 0.0, sign)
        scale = totals[i - i % 2][0]
        shaken.append(quick_two_sum(totals[i][0], totals[i][1] + sign * scale))
    nu = []
    for i in range(2 * RIM):
        nu.append(shaken[i] if i < 2 else add2(double2(shaken[i]), neg2(nu[i % 2])))
    c1 = galerkin(nu)
    q, nu2 = next_moments(nu, c1)
    c2 = galerkin(nu2)

    def proper(v):
        return jnp.broadcast_to(v[0:1], v.shape)

    def energy(d, m):
        total = None
        for i in range(ITERS):
            for j in range(i + 1):
                v = d[i] * d[j] * (m[i + j][0] + m[i - j][0])
                v = 0.5 * v if i == j else v
                total = v if total is None else total + v
        return total

    best1, best2 = [proper(v) for v in c1], [proper(v) for v in c2]
    moved = energy([a - b for a, b in zip(c1, best1)], nu) + energy([a - b for a, b in zip(c2, best2)], nu2)
    size = totals[2 * RIM][0] + energy(best1, nu)
    for i in range(ITERS):
        size = size + 2.0 * best1[i] * totals[2 * RIM + 1 + i][0]
    d = [jnp.zeros_like(c1[0])] * RIM
    for i, u in enumerate(q):
        for j, v in enumerate(best2):
            half = 0.5 * (proper(u) * v)
            d[i + j] = d[i + j] + half
            d[abs(i - j)] = d[abs(i - j)] + half
    for k in range(ITERS):
        d[k] = d[k] + best1[k]
    for k in range(RIM):
        moved = moved + (0.5 * ROUNDING**2) * (d[k] * d[k]) * (nu[0][0] + nu[2 * k][0])
    good = jnp.where(moved <= ALLOWED**2 * size, 1.0, 0.0)
    for shift in (4, 2, 1):
        good = jnp.minimum(good, roll(good, shift, 0))
    return best1, d, good


def fill_weights(conduct, fields, first, last):
    wz, wy, wx, wl, bd, dg = fields
    row = lax.broadcasted_iota(jnp.int32, (SUB, LANES), 0)
    lane = lax.broadcasted_iota(jnp.int32, (SUB, LANES), 1)
    not_last_lane = jnp.where(lane < LANES - 1, FACE, 0.0)
    not_first_lane = jnp.where(lane > 0, FACE, 0.0)
    not_last_row = jnp.where(row < SUB - 1, FACE, 0.0)
    side = jnp.where((lane == 0) | (lane == LANES - 1), FACE, 0.0)
    edge = [side + jnp.where(row == 0, FACE, 0.0), side, side, side + jnp.where(row == SUB - 1, FACE, 0.0)]
    here = conduct(first)
    for e in range(first, last + 1):
        z = e - first
        nxt = [here[1], here[2], here[3], roll(here[0], -1, 0)]
        if e < last:
            above = conduct(e + 1)
        for q in range(4):
            if e < last:
                wz[z, q] = FACE * (here[q] + above[q])
            right = not_last_lane * (here[q] + roll(here[q], -1, 1))
            left = not_first_lane * (here[q] + roll(here[q], 1, 1))
            bound = edge[q] * here[q]
            wx[z, q] = right
            wl[z, q] = left
            wy[z, q] = (FACE if q < 3 else not_last_row) * (here[q] + nxt[q])
            bd[z, q] = bound
            dg[z, q] = KAPPA + (bound + (right + left))
        here = above


def across(load, fields, first, last, emit, residual=False):
    wz, wy, wx, wl, bd, dg = fields
    here = load(first)
    if not residual:
        below = load(first - 1)
        flux_below = [wz[first - 1, k] * (here[k] - below[k]) for k in range(4)]
    for e in range(first, last + 1):
        right = [roll(v, -1, 1) for v in here]
        left = [roll(v, 1, 1) for v in here]
        nxt = [here[1], here[2], here[3], roll(here[0], -1, 0)]
        fy = [wy[e, k] * (nxt[k] - here[k]) for k in range(4)]
        prv = [roll(fy[3], 1, 0), fy[0], fy[1], fy[2]]
        if residual:
            w = [
                bd[e, k] * here[k] - (wx[e, k] * (right[k] - here[k]) - wl[e, k] * (here[k] - left[k])) for k in range(4)
            ]
        else:
            w = [dg[e, k] * here[k] - wx[e, k] * right[k] - wl[e, k] * left[k] for k in range(4)]
        w = [w[k] - fy[k] + prv[k] for k in range(4)]
        if not (residual and e == last):
            above = load(e + 1)
            flux_above = [wz[e, k] * (above[k] - here[k]) for k in range(4)]
            w = [d - f for d, f in zip(w, flux_above)]
        if not (residual and e == first):
            w = [d + f for d, f in zip(w, flux_below)]
        emit(e, here, w)
        if not (residual and e == last):
            here, flux_below = above, flux_above


def planes(ref, *lead, shift=0):
    return lambda e: [ref[(*lead, e - shift, k)] for k in range(4)]


def conductivities(a, low, high):
    depth = a.shape[0]

    def conduct(e):
        if e < RIM:
            return [low(e, q) for q in range(4)]
        if e < RIM + depth:
            return [a[e - RIM, q] for q in range(4)]
        return [high(e - RIM - depth, q) for q in range(4)]

    return conduct


def inside(low, high, below, above):
    one = jnp.ones((SUB, LANES), jnp.float32)
    return {
        below: jnp.where(low(RIM - 1, 0) > 0, one, 0.0),
        above: jnp.where(high(0, 0) > 0, one, 0.0),
    }


def is_odd():
    return lax.axis_index("space") % 2 == 1


def swap(far, near, z, q, odd, tail, head):
    far[z, q] = jnp.where(odd, tail, head)
    near[z, q] = jnp.where(odd, head, tail)


def sides(far, near, odd):
    low = lambda z, q: jnp.where(odd, near[z, q], far[z, q])
    high = lambda z, q: jnp.where(odd, far[z, q], near[z, q])
    return low, high


def stage_kernel(c, f, a, cs, fs, cond, far, near):
    depth = c.shape[0]
    for z in range(depth):
        for q in range(4):
            cs[z, q] = load_rows(c, z, q)
            fs[z, q] = load_rows(f, z, q)
            cond[z, q] = load_rows(a, z, q)
    odd = is_odd()
    for z in range(RIM):
        for q in range(4):
            swap(far, near, z, q, odd, cond[z + depth - RIM, q], cond[z, q])


def open_kernel(c, fix, f, a, x, res, far, near, *fields):
    depth = c.shape[0]
    fill_weights(planes(a), fields, 0, depth - 1)
    for z in range(depth):
        for q in range(4):
            v = c[z, q] + load_rows(fix, z, q)
            x[z, q] = v

    def emit(z, v, image):
        for q in range(4):
            r = SOURCE_WEIGHT * f[z, q] - (1.0 / SIGMA) * image[q]
            res[z, q] = r

    across(planes(x), fields, 0, depth - 1, emit, residual=True)
    odd = is_odd()
    for z in range(RIM):
        for q in range(4):
            swap(far, near, z, q, odd, res[z + depth - RIM, q], res[z, q])
    for q in range(4):
        swap(far, near, RIM, q, odd, x[depth - 1, q], x[0, q])


def basis_kernel(x, res, far, near, a, afar, anear, basis, sums, kept, done, *fields):
    depth = x.shape[0]
    span = depth + 2 * RIM
    low, high = RIM - 1, RIM + depth
    odd = is_odd()
    lo, hi = sides(far, near, odd)
    alo, ahi = sides(afar, anear, odd)
    mask = inside(alo, ahi, low, high)
    fill_weights(conductivities(a, alo, ahi), fields, 0, span - 1)
    wz = fields[0]
    totals = {}

    def take(key, terms):
        s = (terms[0] + terms[1]) + (terms[2] + terms[3])
        if key in totals:
            hi_, e = two_sum(totals[key][0], s)
            totals[key] = (hi_, totals[key][1] + e)
        else:
            totals[key] = (s, jnp.zeros_like(s))

    def store(k, e, new, old):
        if e in mask:
            new = [n * mask[e] for n in new]
        if k < RIM:
            for q in range(4):
                kept[k, e, q] = new[q]
        if RIM <= e < RIM + depth:
            if k < RIM:
                take(2 * k, [n * n for n in new])
            if k > 0:
                take(2 * k - 1, [n * o for n, o in zip(new, old)])
            if k < ITERS:
                v = [x[e - RIM, q] for q in range(4)]
                if k == 0:
                    take(2 * RIM, [u * u for u in v])
                take(2 * RIM + 1 + k, [n * u for n, u in zip(new, v)])

    def copy(k):
        return pltpu.make_async_copy(kept.at[k, pl.ds(RIM, depth)], basis.at[k], done.at[k])

    for e in range(span):
        if e < RIM:
            new = [lo(e, q) for q in range(4)]
        elif e < RIM + depth:
            new = [res[e - RIM, q] for q in range(4)]
        else:
            new = [hi(e - RIM - depth, q) for q in range(4)]
        for face, inner, outer in ((low, 0, lo), (high - 1, depth - 1, hi)):
            if e in (face, face + 1):
                own = (e == face) == (face != low)
                for q in range(4):
                    flux = (1.0 / SIGMA) * wz[face, q] * (x[inner, q] - outer(RIM, q))
                    new[q] = new[q] - flux if own else new[q] + flux
        store(0, e, new, None)
    copy(0).start()
    for k in range(1, RIM + 1):

        def emit(e, v, image, k=k):
            if k == 1:
                new = [0.5 * i for i in image]
            else:
                new = [i - kept[k - 2, e, q] for q, i in enumerate(image)]
            store(k, e, new, v)

        across(planes(kept, k - 1), fields, k, span - 1 - k, emit)
        if k < RIM:
            copy(k).start()
    pack([totals[i] for i in range(TOTALS)], sums)
    for k in range(RIM):
        copy(k).wait()


def states_kernel(gathered, basis, x, out, flag, kept, done):
    depth = x.shape[0]
    copies = [pltpu.make_async_copy(basis.at[k], kept.at[k], done.at[k]) for k in range(RIM)]
    for copy in copies:
        copy.start()
    c, d, good = solve(unpack(gathered))
    flag[0] = good[0, 0].astype(jnp.int32)
    for copy in copies:
        copy.wait()
    for z in range(depth):
        for q in range(4):
            one = two = x[z, q]
            for k in range(RIM):
                part = kept[k, z, q]
                two = two + d[k] * part
                if k < ITERS:
                    one = one + c[k] * part
            out[0, 0, z, pl.ds(q, SUB, stride=4), :] = one
            out[0, 1, z, pl.ds(q, SUB, stride=4), :] = two


def call(kernel, outs, scratch, sent=None, read=None, inputs=0, copies=0, weights=True):
    vmem = pl.BlockSpec(memory_space=pltpu.VMEM)
    hbm = pl.BlockSpec(memory_space=pltpu.HBM)
    smem = pl.BlockSpec(memory_space=pltpu.SMEM)
    own = [pltpu.VMEM(s, jnp.float32) for s in scratch]
    if copies:
        own.append(pltpu.SemaphoreType.DMA((copies,)))
    return lambda fields: pl.pallas_call(
        kernel,
        out_shape=[
            jax.ShapeDtypeStruct((1,), jnp.int32)
            if s is None
            else (pltpu.HBM if i == sent else jax.ShapeDtypeStruct)(s, jnp.float32)
            for i, s in enumerate(outs)
        ],
        in_specs=[hbm if i == read else vmem for i in range(inputs)],
        out_specs=[smem if s is None else hbm if i == sent else vmem for i, s in enumerate(outs)],
        scratch_shapes=own + [pltpu.VMEM(fields, jnp.float32)] * (6 if weights else 0),
        compiler_params=pltpu.CompilerParams(vmem_limit_bytes=20 * 2**20),
    )


def fast(c_points, corrections, conductivity, forcing):
    times, slabs = lax.axis_size("tm"), lax.axis_size("space")
    depth = forcing.shape[0]
    span = depth + 2 * RIM
    tile = (4, SUB, LANES)
    far_pairs = [p for i in range(1, slabs - 1, 2) for p in ((i, i + 1), (i + 1, i))]
    near_pairs = [p for i in range(0, slabs - 1, 2) for p in ((i, i + 1), (i + 1, i))]
    later = [(i, i + 1) for i in range(times - 1)]

    own, sent, rim = (depth, *tile), (RIM + 1, *tile), (RIM, *tile)
    fix = lax.ppermute(corrections[0], "tm", later)
    point, source, cond, far, near = call(
        stage_kernel, [own, own, own, rim, rim], [], inputs=3, weights=False
    )(own)(c_points[0], forcing, conductivity)
    afar = lax.ppermute(far, "space", far_pairs)
    anear = lax.ppermute(near, "space", near_pairs)
    x, res, far, near = call(open_kernel, [own, own, sent, sent], [], inputs=4)(own)(point, fix, source, cond)
    far = lax.ppermute(far, "space", far_pairs)
    near = lax.ppermute(near, "space", near_pairs)
    field = (span, *tile)
    basis, sums = call(
        basis_kernel,
        [(RIM, *own), (slabs, 1, LANES)],
        [(RIM, *field)],
        sent=0,
        inputs=7,
        copies=RIM,
    )(field)(x, res, far, near, cond, afar, anear)
    basis = pltpu.with_memory_space_constraint(basis, pltpu.HBM)
    sums = lax.all_to_all(sums, "space", 0, 0, tiled=True)
    return call(
        states_kernel,
        [(1, STEPS, depth, 4 * SUB, LANES), None],
        [(RIM, *own)],
        read=1,
        inputs=3,
        copies=RIM,
        weights=False,
    )(field)(sums, basis, x)


def copy_for_each(array, axis):
    devices = lax.axis_size(axis)
    return lax.all_to_all(
        jnp.broadcast_to(array[None], (devices, *array.shape)), axis, 0, 0, tiled=True
    )


def over_copies(array, axis):
    return copy_for_each(array, axis).sum(axis=0)


def packed_total(arrays, axis):
    ends = [0]
    for a in arrays:
        ends.append(ends[-1] + a.size)
    subtotal = over_copies(jnp.concatenate([a.ravel() for a in arrays]), axis)
    return tuple((subtotal[b:e].reshape(a.shape) for a, b, e in zip(arrays, ends, ends[1:])))


def extended(cells, sides, width):
    for axis, dim in sides:
        count = lax.axis_size(axis)
        ends = count - 1
        head = lax.slice_in_dim(cells, 0, width, axis=dim)
        tail = lax.slice_in_dim(cells, cells.shape[dim] - width, cells.shape[dim], axis=dim)
        cells = jnp.concatenate(
            [
                lax.ppermute(tail, axis, [(i, (i + 1) % count) for i in range(ends)]),
                cells,
                lax.ppermute(head, axis, [((i + 1) % count, i) for i in range(ends)]),
            ],
            axis=dim,
        )
    return cells


def from_behind(array, axis, by):
    devices = lax.axis_size(axis)
    pairs = [(i, i + by) for i in range(devices) if 0 <= i + by < devices]
    return lax.ppermute(array, axis, pairs)


def neighbours(padded):
    return (
        padded[2:, 1:-1, 1:-1],
        padded[:-2, 1:-1, 1:-1],
        padded[1:-1, 2:, 1:-1],
        padded[1:-1, :-2, 1:-1],
        padded[1:-1, 1:-1, 2:],
        padded[1:-1, 1:-1, :-2],
    )


def faces_of(padded_conductivity):
    centre = padded_conductivity[1:-1, 1:-1, 1:-1]
    return tuple((0.5 * (centre + beside) for beside in neighbours(padded_conductivity)))


def apply_operator(grid_field, padded, face_weights):
    flux_sum = jnp.zeros_like(grid_field)
    for face_weight, beside in zip(face_weights, neighbours(padded)):
        flux_sum = flux_sum + face_weight * (grid_field - beside)
    return grid_field + STEP_RATE * flux_sum


def pair_sums(residual, applied):
    return packed_total((jnp.sum(residual * residual), jnp.sum(residual * applied)), "space")


def plain(c_points, corrections, conductivity, forcing):
    rim_conductivity = extended(conductivity, (("space", 0),), 1)
    face_weights = faces_of(jnp.pad(rim_conductivity, ((0, 0), (1, 1), (1, 1))))

    def operate(grid_field):
        with_planes = extended(grid_field, (("space", 0),), 1)
        padded = jnp.pad(with_planes, ((0, 0), (1, 1), (1, 1)))
        return apply_operator(grid_field, padded, face_weights)

    own_point = c_points[0]
    own_fix = corrections[0]
    prior_fix = from_behind(own_fix, "tm", 1)
    current = own_point + prior_fix
    current_image = operate(current)
    sections = []
    for section in range(STEPS):
        right_side = current + SOURCE_WEIGHT * forcing
        if section > 0:
            current_image = operate(current)
        residual = right_side - current_image
        solution = current
        applied = operate(residual)
        norm_now, product = pair_sums(residual, applied)
        step_length = norm_now / product
        direction = residual
        along_dir = applied
        for sweep in range(ITERS):
            solution = solution + step_length * direction
            if sweep + 1 < ITERS:
                residual = residual - step_length * along_dir
                applied = operate(residual)
                norm_next, product = pair_sums(residual, applied)
                beta_ratio = norm_next / norm_now
                step_length = norm_next / (product - beta_ratio * norm_next / step_length)
                direction = residual + beta_ratio * direction
                along_dir = applied + beta_ratio * along_dir
                norm_now = norm_next
        sections.append(solution)
        current = solution
    return jnp.stack(sections)[None]


def body(c_points, corrections, conductivity, forcing):
    args = (c_points, corrections, conductivity, forcing)
    out, good = fast(*args)
    args, good = lax.optimization_barrier((args, good))
    return lax.cond(good[0] > 0, lambda: out, lambda: plain(*args))


def solution(mesh):
    in_specs = (
        P("tm", "space", None, None),
        P("tm", "space", None, None),
        P("space", None, None),
        P("space", None, None),
    )
    out_specs = P("tm", None, "space", None, None)
    return jax.shard_map(body, mesh=mesh, in_specs=in_specs, out_specs=out_specs, check_vma=False)
```
